8 devices in a mesh: rep: 2 (over y, z), dp: 4 (over x, core).
Axes of the slice: x: 2, y: 2, z: 1, core: 2. Of those that a mesh axis runs over, the one named last changes fastest.
Arguments:
- g_w_gate: bfloat16 [8, 2, 1024, 3072], P(('rep', 'dp')), parts along dimension 0
- g_w_up: bfloat16 [8, 2, 1024, 3072], P(('rep', 'dp')), parts along dimension 0
- g_w_down: bfloat16 [8, 2, 3072, 1024], P(('rep', 'dp')), parts along dimension 0
- w_gate: bfloat16 [2, 1024, 3072], replicated
- w_up: bfloat16 [2, 1024, 3072], replicated
- w_down: bfloat16 [2, 3072, 1024], replicated
- m_w_gate: float32 [2, 1024, 3072], P(None, 'dp')
- m_w_up: float32 [2, 1024, 3072], P(None, 'dp')
- m_w_down: float32 [2, 3072, 1024], P(None, 'dp')
- v_w_gate: float32 [2, 1024, 3072], P(None, 'dp')
- v_w_up: float32 [2, 1024, 3072], P(None, 'dp')
- v_w_down: float32 [2, 3072, 1024], P(None, 'dp')
Outputs:
- output 1: bfloat16 [4, 1024, 3072], P('rep'), parts along dimension 0
- output 2: bfloat16 [4, 1024, 3072], P('rep'), parts along dimension 0
- output 3: bfloat16 [4, 3072, 1024], P('rep'), parts along dimension 0
- output 4: float32 [4, 1024, 3072], P('rep', 'dp'), parts along dimension 0
- output 5: float32 [4, 1024, 3072], P('rep', 'dp'), parts along dimension 0
- output 6: float32 [4, 3072, 1024], P('rep', 'dp'), parts along dimension 0
- output 7: float32 [4, 1024, 3072], P('rep', 'dp'), parts along dimension 0
- output 8: float32 [4, 1024, 3072], P('rep', 'dp'), parts along dimension 0
- output 9: float32 [4, 3072, 1024], P('rep', 'dp'), parts along dimension 0
There are 2 independent parts. The reference program is written for one: setup_inputs(seed, part) draws one part's arguments, and reference() takes and returns one part's arrays. A program takes and returns all parts, laid end to end along the dimension named above; an argument that names none is the same for every part.
All inputs are finite; a program needn't handle non-finite values.
Results may differ from the reference program's by a relative error of at most 0.022.
Values are sent between devices in bfloat16 or wider.
A program may use at most 2 GiB of HBM per device.

```python
import jax
import jax.numpy as jnp
from jax import lax

DEVICES = 4
D = 1024
FF = 3072
LAYERS = 2
NAMES = ("w_gate", "w_up", "w_down")
SHAPES = {"w_gate": (LAYERS, D, FF), "w_up": (LAYERS, D, FF), "w_down": (LAYERS, FF, D)}


def setup_inputs(seed: int = 0, part: int = 0) -> dict:
    kz, *keys = jax.random.split(jax.random.key(seed), 1 + 5 * len(NAMES))
    loud = 2.0 ** jax.random.uniform(kz, (), jnp.float32, -1.0, 1.0)
    drawn = {}
    for name, key, both in zip(NAMES, keys[:3], keys[3:6], strict=True):
        own = jax.random.normal(jax.random.fold_in(key, part), (DEVICES, *SHAPES[name]), jnp.float32)
        shared = jax.random.normal(jax.random.fold_in(both, part), SHAPES[name], jnp.float32)
        drawn["g_" + name] = (loud * (0.7 * shared / DEVICES + 0.7 * own * DEVICES**-0.5)).astype(jnp.bfloat16)
    for name, key in zip(NAMES, keys[6:9], strict=True):
        drawn[name] = (jax.random.normal(key, SHAPES[name], jnp.float32) * SHAPES[name][1] ** -0.5).astype(jnp.bfloat16)
    for name, key in zip(NAMES, keys[9:12], strict=True):
        drawn["m_" + name] = loud * 0.5 * jax.random.normal(key, SHAPES[name], jnp.float32)
    for name, key in zip(NAMES, keys[12:15], strict=True):
        drawn["v_" + name] = loud * loud * jax.random.uniform(key, SHAPES[name], jnp.float32, 0.5, 1.5)
    return drawn


def adamw(w, m, v, g):
    m = 0.9 * m + 0.1 * g
    v = 0.95 * v + 0.05 * g * g
    step = m * lax.rsqrt(v + 1e-8) + 0.1 * w
    return (w - 0.02 * step).astype(jnp.bfloat16), m, v


def reference(g_w_gate, g_w_up, g_w_down, w_gate, w_up, w_down, m_w_gate, m_w_up, m_w_down, v_w_gate, v_w_up, v_w_down):
    def total(terms):
        return lax.scan(lambda so_far, term: (so_far + term.astype(jnp.float32), None), jnp.zeros(terms.shape[1:], jnp.float32), terms)[0]

    gradients = [total(terms).astype(jnp.bfloat16).astype(jnp.float32) for terms in (g_w_gate, g_w_up, g_w_down)]
    new = [
        adamw(w.astype(jnp.float32), m, v, g)
        for w, m, v, g in zip((w_gate, w_up, w_down), (m_w_gate, m_w_up, m_w_down), (v_w_gate, v_w_up, v_w_down), gradients, strict=True)
    ]
    return tuple(one[which] for which in range(3) for one in new)
```

```python
import functools

import jax
import jax.numpy as jnp
from jax import lax
from jax.experimental import pallas as pl
from jax.experimental.pallas import tpu as pltpu
from jax.sharding import PartitionSpec as P


ACROSS = [(0, 2), (2, 0), (1, 3), (3, 1)]
BESIDE = [(0, 1), (1, 0), (2, 3), (3, 2)]

CHUNKS = (
    (0, 0, 0, 64), (0, 0, 64, 192), (0, 1, 0, 256),
    (1, 0, 0, 256), (1, 1, 0, 256),
    (2, 0, 0, 768), (2, 1, 0, 576), (2, 1, 576, 192),
)


MESH = pl.DeviceIdType.MESH


def pair_body(chunk, nears, *refs):
    n = len(nears)
    terms, (both, *near_refs) = refs[:3], refs[3 : 4 + n]
    got, mine, total, got_send, got_recv, in_sem, out_sem, near_send, near_recv = refs[4 + n :]
    which, layer, first, rows = chunk
    me = lax.axis_index("dp")
    partner = {"dp": me ^ 1}
    barrier = pltpu.get_barrier_semaphore()
    pl.semaphore_signal(barrier, inc=1, device_id=partner, device_id_type=MESH)
    pl.semaphore_wait(barrier, 1)

    def block(which, layer, first, rows, owner):
        size = terms[which].shape[2] // 4
        return terms[which].at[0, layer, pl.ds(pl.multiple_of(owner * size + first, 16), rows)]

    tile = pair_tile(rows, terms[which].shape[3])
    count = rows // tile
    fars = [
        pltpu.make_async_remote_copy(
            block(which, layer, first + t * tile, tile, me ^ 3), got.at[pl.ds(t * tile, tile)],
            got_send.at[t], got_recv.at[t], device_id=partner, device_id_type=MESH)
        for t in range(count)
    ]
    owns = [
        pltpu.make_async_copy(block(which, layer, first + t * tile, tile, me ^ 2), mine.at[pl.ds(t * tile, tile)], in_sem.at[t])
        for t in range(count)
    ]
    beside = [
        pltpu.make_async_remote_copy(
            block(*CHUNKS[c], me ^ 1), near_refs[i], near_send.at[i], near_recv.at[i], device_id=partner, device_id_type=MESH)
        for i, c in enumerate(nears)
    ]
    outs = [pltpu.make_async_copy(total.at[pl.ds(t * tile, tile)], both.at[pl.ds(t * tile, tile)], out_sem.at[t]) for t in range(count)]
    for far, own in zip(fars, owns):
        far.start()
        own.start()
    for copy in beside:
        copy.start()
    for t in range(count):
        owns[t].wait()
        fars[t].wait_recv()
        here = pl.ds(t * tile, tile)
        total[here] = (got[here].astype(jnp.float32) + mine[here].astype(jnp.float32)).astype(jnp.bfloat16)
        outs[t].start()
    for t in range(count):
        fars[t].wait_send()
        outs[t].wait()
    for copy in beside:
        copy.wait()


def pair_tile(rows, cols):
    return min(rows, 64 * 3072 // cols)


def pair(terms, index, nears):
    chunk = CHUNKS[index]
    which, _, _, rows = chunk
    cols = terms[which].shape[3]
    count = rows // pair_tile(rows, cols)
    anywhere = pl.BlockSpec(memory_space=pl.ANY)
    shapes = [(rows, cols)] + [(CHUNKS[c][3], terms[CHUNKS[c][0]].shape[3]) for c in nears]
    return pl.pallas_call(
        functools.partial(pair_body, chunk, nears),
        in_specs=[anywhere] * 3,
        out_specs=[anywhere] * len(shapes),
        out_shape=[jax.ShapeDtypeStruct(shape, jnp.bfloat16) for shape in shapes],
        scratch_shapes=[pltpu.VMEM((rows, cols), jnp.bfloat16)] * 3
        + [pltpu.SemaphoreType.DMA((count,))] * 4
        + [pltpu.SemaphoreType.DMA((max(1, len(nears)),))] * 2,
        compiler_params=pltpu.CompilerParams(collective_id=index, has_side_effects=True),
        cost_estimate=pl.CostEstimate(flops=rows * cols, bytes_accessed=10 * rows * cols, transcendentals=0),
        name="pair",
    )(*terms)


def adamw_body(n_alias, me, own, near, far, w, m, v, *rest):
    send, out, m_out, v_out = rest[n_alias:]
    g = own[...].astype(jnp.float32) + near[...].astype(jnp.float32) + far[...].astype(jnp.float32)
    g = g.reshape(m.shape).astype(jnp.bfloat16).astype(jnp.float32)
    m_new = 0.9 * m[...] + 0.1 * g
    v_new = 0.95 * v[...] + 0.05 * g * g
    w_old = w[...].astype(jnp.float32)
    new = (w_old - 0.02 * (m_new * lax.rsqrt(v_new + 1e-8) + 0.1 * w_old)).astype(jnp.bfloat16)
    send[...] = new.reshape(send.shape)
    out[...] = new
    m_out[...] = m_new
    v_out[...] = v_new


def adamw(me, terms, near, far, w, m, v, layer, first, rows, before):
    block, cols = m.shape[1], m.shape[2]
    tile = min(rows, 64 * 3072 // cols)
    at, per = first // tile, block // tile
    mine = pl.BlockSpec((1, tile, cols), lambda i, me: (layer, at + i, 0))
    whole = pl.BlockSpec((1, tile, cols), lambda i, me: (layer, me[0] * per + at + i, 0))
    term = pl.BlockSpec((1, 1, tile, cols), lambda i, me: (0, layer, me[0] * per + at + i, 0))
    chunk = pl.BlockSpec((tile, cols), lambda i, me: (i, 0))
    anywhere = pl.BlockSpec(memory_space=pl.ANY)
    n_alias = len(before)
    size = rows * cols
    return pl.pallas_call(
        functools.partial(adamw_body, n_alias),
        grid_spec=pltpu.PrefetchScalarGridSpec(
            num_scalar_prefetch=1,
            grid=(rows // tile,),
            in_specs=[term, chunk, chunk, whole, mine, mine] + [anywhere] * n_alias,
            out_specs=[chunk, whole, mine, mine],
        ),
        out_shape=[
            jax.ShapeDtypeStruct((rows, cols), jnp.bfloat16),
            jax.ShapeDtypeStruct(w.shape, jnp.bfloat16),
            jax.ShapeDtypeStruct(m.shape, jnp.float32),
            jax.ShapeDtypeStruct(v.shape, jnp.float32),
        ],
        input_output_aliases={7 + i: 1 + i for i in range(n_alias)},
        cost_estimate=pl.CostEstimate(flops=14 * size, bytes_accessed=28 * size, transcendentals=size),
        name="adamw",
    )(me, terms, near, far, w, m, v, *before)


def place_body(layer, first, rows, block, me, beside, across, corner, before, out, held, in_sem, out_sem):
    blocks = (me[0] ^ 1, me[0] ^ 2, me[0] ^ 3)
    ins = [pltpu.make_async_copy(src, held.at[i], in_sem.at[i]) for i, src in enumerate((beside, across, corner))]
    outs = [
        pltpu.make_async_copy(held.at[i], out.at[layer, pl.ds(pl.multiple_of(b * block + first, 16), rows)], out_sem.at[i])
        for i, b in enumerate(blocks)
    ]
    for copy in ins:
        copy.start()
    for came, goes in zip(ins, outs):
        came.wait()
        goes.start()
    for copy in outs:
        copy.wait()


def place(me, pieces, out, layer, first, rows, block):
    cols = out.shape[2]
    anywhere = pl.BlockSpec(memory_space=pl.ANY)
    return pl.pallas_call(
        functools.partial(place_body, layer, first, rows, block),
        in_specs=[pl.BlockSpec(memory_space=pltpu.SMEM)] + [anywhere] * 4,
        out_specs=anywhere,
        out_shape=jax.ShapeDtypeStruct(out.shape, out.dtype),
        input_output_aliases={4: 0},
        scratch_shapes=[
            pltpu.VMEM((3, rows, cols), jnp.bfloat16),
            pltpu.SemaphoreType.DMA((3,)),
            pltpu.SemaphoreType.DMA((3,)),
        ],
        cost_estimate=pl.CostEstimate(flops=3 * rows * cols, bytes_accessed=12 * rows * cols, transcendentals=0),
        name="place",
    )(me, *pieces, out)


def solution(mesh):
    def inner(*arrays):
        terms, weights, m, v = (arrays[i : i + 3] for i in (0, 3, 6, 9))
        me = lax.axis_index("dp").astype(jnp.int32).reshape(1)

        def send(x, to):
            return lax.ppermute(x, "dp", to)

        arrived, near = [], []
        for c in range(len(CHUNKS)):
            both, *more = pair(terms, c, () if c == 0 else (0, 1) if c == 1 else (c,))
            near += more
            arrived.append(send(both, ACROSS))

        state = [() for _ in weights]
        across, beside, corner = [], [], []
        for c, (which, layer, first, rows) in enumerate(CHUNKS):
            one, *state[which] = adamw(
                me, terms[which], near[c], arrived[c], weights[which], m[which], v[which], layer, first, rows, tuple(state[which]))
            across.append(send(one, ACROSS))
            beside.append(send(one, BESIDE))
        for c, (which, layer, first, rows) in enumerate(CHUNKS):
            corner.append(send(across[c], BESIDE))
        for c, (which, layer, first, rows) in enumerate(CHUNKS):
            state[which][0] = place(me, (beside[c], across[c], corner[c]), state[which][0], layer, first, rows, m[which].shape[1])
        return tuple(state[which][i] for i in range(3) for which in range(3))

    all_of, cut_rows = P(None, None, None), P(None, "dp", None)
    return jax.shard_map(
        inner,
        mesh=mesh,
        in_specs=(P(("rep", "dp"), None, None, None),) * 3 + (all_of,) * 3 + (cut_rows,) * 6,
        out_specs=(P("rep", None, None),) * 3 + (P("rep", "dp", None),) * 6,
        check_vma=False,
    )
```

```python
import functools
import math

import jax
import jax.numpy as jnp
from jax import lax
from jax.experimental import pallas as pl
from jax.experimental.pallas import tpu as pltpu
from jax.sharding import PartitionSpec as P


ACROSS = [(0, 2), (2, 0), (1, 3), (3, 1)]
BESIDE = [(0, 1), (1, 0), (2, 3), (3, 2)]

CHUNKS = (
    (0, 0, 0, 32), (0, 0, 32, 96), (0, 0, 128, 128), (0, 1, 0, 256),
    (1, 0, 0, 256), (1, 1, 0, 256),
    (2, 0, 0, 768), (2, 1, 0, 384), (2, 1, 384, 192), (2, 1, 576, 96), (2, 1, 672, 96),
)
MESH = pl.DeviceIdType.MESH


def pair_body(chunk, nears, *refs):
    n = len(nears)
    terms, (both, *near_refs) = refs[:3], refs[3 : 4 + n]
    got, mine, total, got_send, got_recv, in_sem, out_sem, near_send, near_recv = refs[4 + n :]
    which, layer, first, rows = chunk
    me = lax.axis_index("dp")
    partner = {"dp": me ^ 1}
    barrier = pltpu.get_barrier_semaphore()
    pl.semaphore_signal(barrier, inc=1, device_id=partner, device_id_type=MESH)

    def block(which, layer, first, rows, owner):
        size = terms[which].shape[2] // 4
        return terms[which].at[0, layer, pl.ds(pl.multiple_of(owner * size + first, 16), rows)]

    tile = pair_tile(rows, terms[which].shape[3])
    count = rows // tile
    owns = [
        pltpu.make_async_copy(block(which, layer, first + t * tile, tile, me ^ 2), mine.at[pl.ds(t * tile, tile)], in_sem.at[t])
        for t in range(count)
    ]
    fars = [
        pltpu.make_async_remote_copy(
            block(which, layer, first + t * tile, tile, me ^ 3), got.at[pl.ds(t * tile, tile)],
            got_send.at[t], got_recv.at[t], device_id=partner, device_id_type=MESH)
        for t in range(count)
    ]
    beside = [
        pltpu.make_async_remote_copy(
            block(*CHUNKS[c], me ^ 1), near_refs[i], near_send.at[i], near_recv.at[i], device_id=partner, device_id_type=MESH)
        for i, c in enumerate(nears)
    ]
    outs = [pltpu.make_async_copy(total.at[pl.ds(t * tile, tile)], both.at[pl.ds(t * tile, tile)], out_sem.at[t]) for t in range(count)]
    pl.semaphore_wait(barrier, 1)
    for far, own in zip(fars, owns):
        far.start()
        own.start()
    for copy in beside:
        copy.start()
    for t in range(count):
        owns[t].wait()
        fars[t].wait_recv()
        here = pl.ds(t * tile, tile)
        total[here] = (got[here].astype(jnp.float32) + mine[here].astype(jnp.float32)).astype(jnp.bfloat16)
        outs[t].start()
    for t in range(count):
        fars[t].wait_send()
        outs[t].wait()
    for copy in beside:
        copy.wait()


def first_pair_body(chunk, terms, both, got, mine, send_sem, recv_sem, in_sem):
    _, layer, first, rows = chunk
    me = lax.axis_index("dp")
    partner = {"dp": me ^ 1}
    barrier = pltpu.get_barrier_semaphore()
    pl.semaphore_signal(barrier, inc=1, device_id=partner, device_id_type=MESH)

    def block(owner):
        size = terms.shape[2] // 4
        return terms.at[0, layer, pl.ds(pl.multiple_of(owner * size + first, 16), rows)]

    own = pltpu.make_async_copy(block(me ^ 2), mine, in_sem)
    far = pltpu.make_async_remote_copy(block(me ^ 3), got, send_sem, recv_sem, device_id=partner, device_id_type=MESH)
    own.start()
    pl.semaphore_wait(barrier, 1)
    far.start()
    own.wait()
    far.wait_recv()
    both[...] = (got[...].astype(jnp.float32) + mine[...].astype(jnp.float32)).astype(jnp.bfloat16)
    far.wait_send()


def first_pair(terms):
    which, _, _, rows = CHUNKS[0]
    cols = terms[which].shape[3]
    return pl.pallas_call(
        functools.partial(first_pair_body, CHUNKS[0]),
        in_specs=[pl.BlockSpec(memory_space=pltpu.HBM)],
        out_specs=pl.BlockSpec(memory_space=pltpu.VMEM),
        out_shape=jax.ShapeDtypeStruct((rows, cols), jnp.bfloat16),
        scratch_shapes=[pltpu.VMEM((rows, cols), jnp.bfloat16)] * 2 + [pltpu.SemaphoreType.DMA] * 3,
        compiler_params=pltpu.CompilerParams(collective_id=0, has_side_effects=True, vmem_limit_bytes=52 * 2**20),
        cost_estimate=pl.CostEstimate(flops=rows * cols, bytes_accessed=8 * rows * cols, transcendentals=0),
        name="first_pair",
    )(terms[which])


def pair_tile(rows, cols):
    return math.gcd(rows, 64 * 3072 // cols)


def pair(terms, index, nears):
    chunk = CHUNKS[index]
    which, _, _, rows = chunk
    cols = terms[which].shape[3]
    count = rows // pair_tile(rows, cols)
    anywhere = pl.BlockSpec(memory_space=pl.ANY)
    shapes = [(rows, cols)] + [(CHUNKS[c][3], terms[CHUNKS[c][0]].shape[3]) for c in nears]
    return pl.pallas_call(
        functools.partial(pair_body, chunk, nears),
        in_specs=[anywhere] * 3,
        out_specs=[anywhere] * len(shapes),
        out_shape=[jax.ShapeDtypeStruct(shape, jnp.bfloat16) for shape in shapes],
        scratch_shapes=[pltpu.VMEM((rows, cols), jnp.bfloat16)] * 3
        + [pltpu.SemaphoreType.DMA((count,))] * 4
        + [pltpu.SemaphoreType.DMA((max(1, len(nears)),))] * 2,
        compiler_params=pltpu.CompilerParams(collective_id=index, has_side_effects=True),
        cost_estimate=pl.CostEstimate(flops=rows * cols, bytes_accessed=10 * rows * cols, transcendentals=0),
        name="pair",
    )(*terms)


def adamw_body(n_alias, me, own, near, far, w, m, v, *rest):
    send, out, m_out, v_out = rest[n_alias:]
    g = own[...].astype(jnp.float32) + near[...].astype(jnp.float32) + far[...].astype(jnp.float32)
    g = g.reshape(m.shape).astype(jnp.bfloat16).astype(jnp.float32)
    m_new = 0.9 * m[...] + 0.1 * g
    v_new = 0.95 * v[...] + 0.05 * g * g
    w_old = w[...].astype(jnp.float32)
    new = (w_old - 0.02 * (m_new * lax.rsqrt(v_new + 1e-8) + 0.1 * w_old)).astype(jnp.bfloat16)
    send[...] = new.reshape(send.shape)
    out[...] = new
    m_out[...] = m_new
    v_out[...] = v_new


def adamw(me, terms, near, far, w, m, v, layer, first, rows, before):
    block, cols = m.shape[1], m.shape[2]
    tile = math.gcd(rows, first, block, 64 * 3072 // cols)
    at, per = first // tile, block // tile
    mine = pl.BlockSpec((1, tile, cols), lambda i, me: (layer, at + i, 0))
    whole = pl.BlockSpec((1, tile, cols), lambda i, me: (layer, me[0] * per + at + i, 0))
    term = pl.BlockSpec((1, 1, tile, cols), lambda i, me: (0, layer, me[0] * per + at + i, 0))
    chunk = pl.BlockSpec((tile, cols), lambda i, me: (i, 0))
    anywhere = pl.BlockSpec(memory_space=pl.ANY)
    n_alias = len(before)
    size = rows * cols
    return pl.pallas_call(
        functools.partial(adamw_body, n_alias),
        grid_spec=pltpu.PrefetchScalarGridSpec(
            num_scalar_prefetch=1,
            grid=(rows // tile,),
            in_specs=[term, chunk, chunk, whole, mine, mine] + [anywhere] * n_alias,
            out_specs=[chunk, whole, mine, mine],
        ),
        out_shape=[
            jax.ShapeDtypeStruct((rows, cols), jnp.bfloat16),
            jax.ShapeDtypeStruct(w.shape, jnp.bfloat16),
            jax.ShapeDtypeStruct(m.shape, jnp.float32),
            jax.ShapeDtypeStruct(v.shape, jnp.float32),
        ],
        input_output_aliases={7 + i: 1 + i for i in range(n_alias)},
        cost_estimate=pl.CostEstimate(flops=14 * size, bytes_accessed=28 * size, transcendentals=size),
        name="adamw",
    )(me, terms, near, far, w, m, v, *before)


def place_body(layer, first, rows, block, me, beside, across, corner, before, out, sem):
    copies = [
        pltpu.make_async_copy(src, out.at[layer, pl.ds(pl.multiple_of((me[0] ^ other) * block + first, 16), rows)], sem.at[i])
        for i, (src, other) in enumerate(((beside, 1), (across, 2), (corner, 3)))
    ]
    for copy in copies:
        copy.start()
    for copy in copies:
        copy.wait()


def place(me, pieces, out, layer, first, rows, block):
    cols = out.shape[2]
    anywhere = pl.BlockSpec(memory_space=pl.ANY)
    return pl.pallas_call(
        functools.partial(place_body, layer, first, rows, block),
        in_specs=[pl.BlockSpec(memory_space=pltpu.SMEM)] + [pl.BlockSpec(memory_space=pltpu.VMEM)] * 3 + [anywhere],
        out_specs=anywhere,
        out_shape=jax.ShapeDtypeStruct(out.shape, out.dtype),
        input_output_aliases={4: 0},
        scratch_shapes=[pltpu.SemaphoreType.DMA((3,))],
        compiler_params=pltpu.CompilerParams(vmem_limit_bytes=16 * 2**20),
        cost_estimate=pl.CostEstimate(flops=3 * rows * cols, bytes_accessed=12 * rows * cols, transcendentals=0),
        name="place",
    )(me, *pieces, out)


def solution(mesh):
    def inner(*arrays):
        terms, weights, m, v = (arrays[i : i + 3] for i in (0, 3, 6, 9))
        me = lax.axis_index("dp").astype(jnp.int32).reshape(1)

        def send(x, to):
            return lax.ppermute(x, "dp", to)

        arrived, near = [], []
        for c in range(len(CHUNKS)):
            both, *more = pair(terms, c, (0, 1) if c == 1 else (c,)) if c else (first_pair(terms),)
            near += more
            arrived.append(send(both, ACROSS))

        state = [() for _ in weights]
        across, beside, corner = [], [], []
        for c, (which, layer, first, rows) in enumerate(CHUNKS):
            one, *state[which] = adamw(
                me, terms[which], near[c], arrived[c], weights[which], m[which], v[which], layer, first, rows, tuple(state[which]))
            across.append(send(one, ACROSS))
            beside.append(send(one, BESIDE))
        for c, (which, layer, first, rows) in enumerate(CHUNKS):
            corner.append(send(across[c], BESIDE))
        for c, (which, layer, first, rows) in enumerate(CHUNKS):
            state[which][0] = place(me, (beside[c], across[c], corner[c]), state[which][0], layer, first, rows, m[which].shape[1])
        return tuple(state[which][i] for i in range(3) for which in range(3))

    all_of, cut_rows = P(None, None, None), P(None, "dp", None)
    return jax.shard_map(
        inner,
        mesh=mesh,
        in_specs=(P(("rep", "dp"), None, None, None),) * 3 + (all_of,) * 3 + (cut_rows,) * 6,
        out_specs=(P("rep", None, None),) * 3 + (P("rep", "dp", None),) * 6,
        check_vma=False,
    )
```

```python
import functools
import math

import jax
import jax.numpy as jnp
from jax import lax
from jax.experimental import pallas as pl
from jax.experimental.pallas import tpu as pltpu
from jax.sharding import PartitionSpec as P


ACROSS = [(0, 2), (2, 0), (1, 3), (3, 1)]
BESIDE = [(0, 1), (1, 0), (2, 3), (3, 2)]

CHUNKS = (
    (0, 0, 0, 48), (0, 0, 48, 80), (0, 0, 128, 128), (0, 1, 0, 256),
    (1, 0, 0, 256), (1, 1, 0, 256),
    (2, 0, 0, 768), (2, 1, 0, 384), (2, 1, 384, 240), (2, 1, 624, 96), (2, 1, 720, 48),
)
LAST = len(CHUNKS) - 1
MESH = pl.DeviceIdType.MESH


def pair_body(chunk, nears, *refs):
    n = len(nears)
    terms, (both, *near_refs) = refs[:3], refs[3 : 4 + n]
    got, mine, total, got_send, got_recv, in_sem, out_sem, near_send, near_recv = refs[4 + n :]
    which, layer, first, rows = chunk
    me = lax.axis_index("dp")
    partner = {"dp": me ^ 1}
    barrier = pltpu.get_barrier_semaphore()
    pl.semaphore_signal(barrier, inc=1, device_id=partner, device_id_type=MESH)

    def block(which, layer, first, rows, owner):
        size = terms[which].shape[2] // 4
        return terms[which].at[0, layer, pl.ds(pl.multiple_of(owner * size + first, 16), rows)]

    tile = pair_tile(rows, terms[which].shape[3])
    count = rows // tile
    owns = [
        pltpu.make_async_copy(block(which, layer, first + t * tile, tile, me ^ 2), mine.at[pl.ds(t * tile, tile)], in_sem.at[t])
        for t in range(count)
    ]
    fars = [
        pltpu.make_async_remote_copy(
            block(which, layer, first + t * tile, tile, me ^ 3), got.at[pl.ds(t * tile, tile)],
            got_send.at[t], got_recv.at[t], device_id=partner, device_id_type=MESH)
        for t in range(count)
    ]
    beside = [
        pltpu.make_async_remote_copy(
            block(*CHUNKS[c], me ^ 1), near_refs[i], near_send.at[i], near_recv.at[i], device_id=partner, device_id_type=MESH)
        for i, c in enumerate(nears)
    ]
    outs = [pltpu.make_async_copy(total.at[pl.ds(t * tile, tile)], both.at[pl.ds(t * tile, tile)], out_sem.at[t]) for t in range(count)]
    pl.semaphore_wait(barrier, 1)
    for far, own in zip(fars, owns):
        far.start()
        own.start()
    for copy in beside:
        copy.start()
    for t in range(count):
        owns[t].wait()
        fars[t].wait_recv()
        here = pl.ds(t * tile, tile)
        total[here] = (got[here].astype(jnp.float32) + mine[here].astype(jnp.float32)).astype(jnp.bfloat16)
        outs[t].start()
    for t in range(count):
        fars[t].wait_send()
        outs[t].wait()
    for copy in beside:
        copy.wait()


def first_pair_body(chunk, terms, both, got, mine, send_sem, recv_sem, in_sem):
    _, layer, first, rows = chunk
    me = lax.axis_index("dp")
    partner = {"dp": me ^ 1}
    barrier = pltpu.get_barrier_semaphore()
    pl.semaphore_signal(barrier, inc=1, device_id=partner, device_id_type=MESH)

    def block(owner):
        size = terms.shape[2] // 4
        return terms.at[0, layer, pl.ds(pl.multiple_of(owner * size + first, 16), rows)]

    own = pltpu.make_async_copy(block(me ^ 2), mine, in_sem)
    far = pltpu.make_async_remote_copy(block(me ^ 3), got, send_sem, recv_sem, device_id=partner, device_id_type=MESH)
    own.start()
    pl.semaphore_wait(barrier, 1)
    far.start()
    own.wait()
    far.wait_recv()
    both[...] = (got[...].astype(jnp.float32) + mine[...].astype(jnp.float32)).astype(jnp.bfloat16)
    far.wait_send()


def first_pair(terms):
    which, _, _, rows = CHUNKS[0]
    cols = terms[which].shape[3]
    return pl.pallas_call(
        functools.partial(first_pair_body, CHUNKS[0]),
        in_specs=[pl.BlockSpec(memory_space=pltpu.HBM)],
        out_specs=pl.BlockSpec(memory_space=pltpu.VMEM),
        out_shape=jax.ShapeDtypeStruct((rows, cols), jnp.bfloat16),
        scratch_shapes=[pltpu.VMEM((rows, cols), jnp.bfloat16)] * 2 + [pltpu.SemaphoreType.DMA] * 3,
        compiler_params=pltpu.CompilerParams(collective_id=0, has_side_effects=True, vmem_limit_bytes=52 * 2**20),
        cost_estimate=pl.CostEstimate(flops=rows * cols, bytes_accessed=8 * rows * cols, transcendentals=0),
        name="first_pair",
    )(terms[which])


def pair_tile(rows, cols):
    return math.gcd(rows, 64 * 3072 // cols)


def pair(terms, index, nears):
    chunk = CHUNKS[index]
    which, _, _, rows = chunk
    cols = terms[which].shape[3]
    count = rows // pair_tile(rows, cols)
    anywhere = pl.BlockSpec(memory_space=pl.ANY)
    shapes = [(rows, cols)] + [(CHUNKS[c][3], terms[CHUNKS[c][0]].shape[3]) for c in nears]
    return pl.pallas_call(
        functools.partial(pair_body, chunk, nears),
        in_specs=[anywhere] * 3,
        out_specs=[anywhere] * len(shapes),
        out_shape=[jax.ShapeDtypeStruct(shape, jnp.bfloat16) for shape in shapes],
        scratch_shapes=[pltpu.VMEM((rows, cols), jnp.bfloat16)] * 3
        + [pltpu.SemaphoreType.DMA((count,))] * 4
        + [pltpu.SemaphoreType.DMA((max(1, len(nears)),))] * 2,
        compiler_params=pltpu.CompilerParams(collective_id=index, has_side_effects=True),
        cost_estimate=pl.CostEstimate(flops=rows * cols, bytes_accessed=10 * rows * cols, transcendentals=0),
        name="pair",
    )(*terms)


def adamw_body(n_alias, me, own, near, far, w, m, v, *rest):
    send, out, m_out, v_out = rest[n_alias:]
    g = own[...].astype(jnp.float32) + near[...].astype(jnp.float32) + far[...].astype(jnp.float32)
    g = g.reshape(m.shape).astype(jnp.bfloat16).astype(jnp.float32)
    m_new = 0.9 * m[...] + 0.1 * g
    v_new = 0.95 * v[...] + 0.05 * g * g
    w_old = w[...].astype(jnp.float32)
    new = (w_old - 0.02 * (m_new * lax.rsqrt(v_new + 1e-8) + 0.1 * w_old)).astype(jnp.bfloat16)
    send[...] = new.reshape(send.shape)
    out[...] = new
    m_out[...] = m_new
    v_out[...] = v_new


def adamw(me, terms, near, far, w, m, v, layer, first, rows, before):
    block, cols = m.shape[1], m.shape[2]
    tile = math.gcd(rows, first, block, 64 * 3072 // cols)
    at, per = first // tile, block // tile
    mine = pl.BlockSpec((1, tile, cols), lambda i, me: (layer, at + i, 0))
    whole = pl.BlockSpec((1, tile, cols), lambda i, me: (layer, me[0] * per + at + i, 0))
    term = pl.BlockSpec((1, 1, tile, cols), lambda i, me: (0, layer, me[0] * per + at + i, 0))
    chunk = pl.BlockSpec((tile, cols), lambda i, me: (i, 0))
    anywhere = pl.BlockSpec(memory_space=pl.ANY)
    n_alias = len(before)
    size = rows * cols
    return pl.pallas_call(
        functools.partial(adamw_body, n_alias),
        grid_spec=pltpu.PrefetchScalarGridSpec(
            num_scalar_prefetch=1,
            grid=(rows // tile,),
            in_specs=[term, chunk, chunk, whole, mine, mine] + [anywhere] * n_alias,
            out_specs=[chunk, whole, mine, mine],
        ),
        out_shape=[
            jax.ShapeDtypeStruct((rows, cols), jnp.bfloat16),
            jax.ShapeDtypeStruct(w.shape, jnp.bfloat16),
            jax.ShapeDtypeStruct(m.shape, jnp.float32),
            jax.ShapeDtypeStruct(v.shape, jnp.float32),
        ],
        input_output_aliases={7 + i: 1 + i for i in range(n_alias)},
        cost_estimate=pl.CostEstimate(flops=14 * size, bytes_accessed=28 * size, transcendentals=size),
        name="adamw",
    )(me, terms, near, far, w, m, v, *before)


def place_body(chunks, block, me, *refs):
    pieces, (_, out, sem) = refs[: 3 * len(chunks)], refs[3 * len(chunks) :]
    copies = []
    for i, src in enumerate(pieces):
        _, layer, first, rows = chunks[i // 3]
        owner = me[0] ^ (1 + i % 3)
        copies.append(pltpu.make_async_copy(src, out.at[layer, pl.ds(pl.multiple_of(owner * block + first, 16), rows)], sem.at[i]))
    for copy in copies:
        copy.start()
    for copy in copies:
        copy.wait()


def place(me, chunks, pieces, out, block):
    cols = out.shape[2]
    size = sum(chunk[3] for chunk in chunks) * cols
    anywhere = pl.BlockSpec(memory_space=pl.ANY)
    n = 3 * len(chunks)
    return pl.pallas_call(
        functools.partial(place_body, chunks, block),
        in_specs=[pl.BlockSpec(memory_space=pltpu.SMEM)] + [pl.BlockSpec(memory_space=pltpu.VMEM)] * n + [anywhere],
        out_specs=anywhere,
        out_shape=jax.ShapeDtypeStruct(out.shape, out.dtype),
        input_output_aliases={1 + n: 0},
        scratch_shapes=[pltpu.SemaphoreType.DMA((n,))],
        compiler_params=pltpu.CompilerParams(vmem_limit_bytes=16 * 2**20),
        cost_estimate=pl.CostEstimate(flops=3 * size, bytes_accessed=12 * size, transcendentals=0),
        name="place",
    )(me, *pieces, out)


def solution(mesh):
    def inner(*arrays):
        terms, weights, m, v = (arrays[i : i + 3] for i in (0, 3, 6, 9))
        me = lax.axis_index("dp").astype(jnp.int32).reshape(1)

        def send(x, to):
            return lax.ppermute(x, "dp", to)

        arrived, near = [], []
        for c in range(len(CHUNKS)):
            both, *more = pair(terms, c, () if c == 1 else (0, 1, 2) if c == 2 else (c,)) if c else (first_pair(terms),)
            near += more
            arrived.append(send(both, ACROSS))

        state = [() for _ in weights]
        across, beside, corner = [], [], []
        for c, (which, layer, first, rows) in enumerate(CHUNKS):
            one, *state[which] = adamw(
                me, terms[which], near[c], arrived[c], weights[which], m[which], v[which], layer, first, rows, tuple(state[which]))
            across.append(send(one, ACROSS))
            beside.append(send(one, BESIDE))
        for c in range(len(CHUNKS)):
            corner.append(send(across[c], BESIDE))
        for c in range(LAST):
            which = CHUNKS[c][0]
            together = (c,) if c < LAST - 1 else (c, LAST)
            pieces = [got[i] for i in together for got in (beside, across, corner)]
            state[which][0] = place(me, [CHUNKS[i] for i in together], pieces, state[which][0], m[which].shape[1])
        return tuple(state[which][i] for i in range(3) for which in range(3))

    all_of, cut_rows = P(None, None, None), P(None, "dp", None)
    return jax.shard_map(
        inner,
        mesh=mesh,
        in_specs=(P(("rep", "dp"), None, None, None),) * 3 + (all_of,) * 3 + (cut_rows,) * 6,
        out_specs=(P("rep", None, None),) * 3 + (P("rep", "dp", None),) * 6,
        check_vma=False,
    )
```

```python
import functools
import math

import jax
import jax.numpy as jnp
from jax import lax
from jax.experimental import pallas as pl
from jax.experimental.pallas import tpu as pltpu
from jax.sharding import PartitionSpec as P


ACROSS = [(0, 2), (2, 0), (1, 3), (3, 1)]
BESIDE = [(0, 1), (1, 0), (2, 3), (3, 2)]

CHUNKS = (
    (0, 0, 0, 48), (0, 0, 48, 80), (0, 0, 128, 128), (0, 1, 0, 256),
    (1, 0, 0, 256), (1, 1, 0, 256),
    (2, 0, 0, 768), (2, 1, 0, 384), (2, 1, 384, 240), (2, 1, 624, 96), (2, 1, 720, 48),
)
LAST = len(CHUNKS) - 1
MESH = pl.DeviceIdType.MESH


def pair_body(chunk, nears, *refs):
    n = len(nears)
    terms, (both, *near_refs) = refs[:3], refs[3 : 4 + n]
    got, mine, total, got_send, got_recv, in_sem, out_sem, near_send, near_recv = refs[4 + n :]
    which, layer, first, rows = chunk
    me = lax.axis_index("dp")
    partner = {"dp": me ^ 1}
    barrier = pltpu.get_barrier_semaphore()
    pl.semaphore_signal(barrier, inc=1, device_id=partner, device_id_type=MESH)

    def block(which, layer, first, rows, owner):
        size = terms[which].shape[2] // 4
        return terms[which].at[0, layer, pl.ds(pl.multiple_of(owner * size + first, 16), rows)]

    tile = rows
    count = rows // tile
    owns = [
        pltpu.make_async_copy(block(which, layer, first + t * tile, tile, me ^ 2), mine.at[pl.ds(t * tile, tile)], in_sem.at[t])
        for t in range(count)
    ]
    fars = [
        pltpu.make_async_remote_copy(
            block(which, layer, first + t * tile, tile, me ^ 3), got.at[pl.ds(t * tile, tile)],
            got_send.at[t], got_recv.at[t], device_id=partner, device_id_type=MESH)
        for t in range(count)
    ]
    beside = [
        pltpu.make_async_remote_copy(
            block(*CHUNKS[c], me ^ 1), near_refs[i], near_send.at[i], near_recv.at[i], device_id=partner, device_id_type=MESH)
        for i, c in enumerate(nears)
    ]
    outs = [pltpu.make_async_copy(total.at[pl.ds(t * tile, tile)], both.at[pl.ds(t * tile, tile)], out_sem.at[t]) for t in range(count)]
    pl.semaphore_wait(barrier, 1)
    for far, own in zip(fars, owns):
        far.start()
        own.start()
    for copy in beside:
        copy.start()
    for t in range(count):
        owns[t].wait()
        fars[t].wait_recv()
        here = pl.ds(t * tile, tile)
        total[here] = (got[here].astype(jnp.float32) + mine[here].astype(jnp.float32)).astype(jnp.bfloat16)
        outs[t].start()
    for t in range(count):
        fars[t].wait_send()
        outs[t].wait()
    for copy in beside:
        copy.wait()


def first_pair_body(chunk, terms, both, got, mine, send_sem, recv_sem, in_sem):
    _, layer, first, rows = chunk
    me = lax.axis_index("dp")
    partner = {"dp": me ^ 1}
    barrier = pltpu.get_barrier_semaphore()
    pl.semaphore_signal(barrier, inc=1, device_id=partner, device_id_type=MESH)

    def block(owner):
        size = terms.shape[2] // 4
        return terms.at[0, layer, pl.ds(pl.multiple_of(owner * size + first, 16), rows)]

    own = pltpu.make_async_copy(block(me ^ 2), mine, in_sem)
    far = pltpu.make_async_remote_copy(block(me ^ 3), got, send_sem, recv_sem, device_id=partner, device_id_type=MESH)
    own.start()
    pl.semaphore_wait(barrier, 1)
    far.start()
    own.wait()
    far.wait_recv()
    both[...] = (got[...].astype(jnp.float32) + mine[...].astype(jnp.float32)).astype(jnp.bfloat16)
    far.wait_send()


def first_pair(terms):
    which, _, _, rows = CHUNKS[0]
    cols = terms[which].shape[3]
    return pl.pallas_call(
        functools.partial(first_pair_body, CHUNKS[0]),
        in_specs=[pl.BlockSpec(memory_space=pltpu.HBM)],
        out_specs=pl.BlockSpec(memory_space=pltpu.VMEM),
        out_shape=jax.ShapeDtypeStruct((rows, cols), jnp.bfloat16),
        scratch_shapes=[pltpu.VMEM((rows, cols), jnp.bfloat16)] * 2 + [pltpu.SemaphoreType.DMA] * 3,
        compiler_params=pltpu.CompilerParams(collective_id=0, has_side_effects=True, vmem_limit_bytes=52 * 2**20),
        cost_estimate=pl.CostEstimate(flops=rows * cols, bytes_accessed=8 * rows * cols, transcendentals=0),
        name="first_pair",
    )(terms[which])


def pair(terms, index, nears):
    chunk = CHUNKS[index]
    which, _, _, rows = chunk
    cols = terms[which].shape[3]
    count = rows // rows
    anywhere = pl.BlockSpec(memory_space=pl.ANY)
    shapes = [(rows, cols)] + [(CHUNKS[c][3], terms[CHUNKS[c][0]].shape[3]) for c in nears]
    return pl.pallas_call(
        functools.partial(pair_body, chunk, nears),
        in_specs=[anywhere] * 3,
        out_specs=[anywhere] * len(shapes),
        out_shape=[jax.ShapeDtypeStruct(shape, jnp.bfloat16) for shape in shapes],
        scratch_shapes=[pltpu.VMEM((rows, cols), jnp.bfloat16)] * 3
        + [pltpu.SemaphoreType.DMA((count,))] * 4
        + [pltpu.SemaphoreType.DMA((max(1, len(nears)),))] * 2,
        compiler_params=pltpu.CompilerParams(collective_id=index, has_side_effects=True),
        cost_estimate=pl.CostEstimate(flops=rows * cols, bytes_accessed=10 * rows * cols, transcendentals=0),
        name="pair",
    )(*terms)


def adamw_body(n_alias, me, own, near, far, w, m, v, *rest):
    send, out, m_out, v_out = rest[n_alias:]
    g = own[...].astype(jnp.float32) + near[...].astype(jnp.float32) + far[...].astype(jnp.float32)
    g = g.reshape(m.shape).astype(jnp.bfloat16).astype(jnp.float32)
    m_new = 0.9 * m[...] + 0.1 * g
    v_new = 0.95 * v[...] + 0.05 * g * g
    w_old = w[...].astype(jnp.float32)
    new = (w_old - 0.02 * (m_new * lax.rsqrt(v_new + 1e-8) + 0.1 * w_old)).astype(jnp.bfloat16)
    send[...] = new.reshape(send.shape)
    out[...] = new
    m_out[...] = m_new
    v_out[...] = v_new


def adamw(me, terms, near, far, w, m, v, layer, first, rows, before):
    block, cols = m.shape[1], m.shape[2]
    tile = math.gcd(rows, first, block, 128 * 3072 // cols)
    at, per = first // tile, block // tile
    mine = pl.BlockSpec((1, tile, cols), lambda i, me: (layer, at + i, 0))
    whole = pl.BlockSpec((1, tile, cols), lambda i, me: (layer, me[0] * per + at + i, 0))
    term = pl.BlockSpec((1, 1, tile, cols), lambda i, me: (0, layer, me[0] * per + at + i, 0))
    chunk = pl.BlockSpec((tile, cols), lambda i, me: (i, 0))
    anywhere = pl.BlockSpec(memory_space=pl.ANY)
    n_alias = len(before)
    size = rows * cols
    return pl.pallas_call(
        functools.partial(adamw_body, n_alias),
        grid_spec=pltpu.PrefetchScalarGridSpec(
            num_scalar_prefetch=1,
            grid=(rows // tile,),
            in_specs=[term, chunk, chunk, whole, mine, mine] + [anywhere] * n_alias,
            out_specs=[chunk, whole, mine, mine],
        ),
        out_shape=[
            jax.ShapeDtypeStruct((rows, cols), jnp.bfloat16),
            jax.ShapeDtypeStruct(w.shape, jnp.bfloat16),
            jax.ShapeDtypeStruct(m.shape, jnp.float32),
            jax.ShapeDtypeStruct(v.shape, jnp.float32),
        ],
        input_output_aliases={7 + i: 1 + i for i in range(n_alias)},
        cost_estimate=pl.CostEstimate(flops=14 * size, bytes_accessed=28 * size, transcendentals=size),
        name="adamw",
    )(me, terms, near, far, w, m, v, *before)


def place_body(chunks, block, me, *refs):
    pieces, (_, out, sem) = refs[: 3 * len(chunks)], refs[3 * len(chunks) :]
    copies = []
    for i, src in enumerate(pieces):
        _, layer, first, rows = chunks[i // 3]
        owner = me[0] ^ (1 + i % 3)
        copies.append(pltpu.make_async_copy(src, out.at[layer, pl.ds(pl.multiple_of(owner * block + first, 16), rows)], sem.at[i]))
    for copy in copies:
        copy.start()
    for copy in copies:
        copy.wait()


def place(me, chunks, pieces, out, block):
    cols = out.shape[2]
    size = sum(chunk[3] for chunk in chunks) * cols
    anywhere = pl.BlockSpec(memory_space=pl.ANY)
    n = 3 * len(chunks)
    return pl.pallas_call(
        functools.partial(place_body, chunks, block),
        in_specs=[pl.BlockSpec(memory_space=pltpu.SMEM)] + [pl.BlockSpec(memory_space=pltpu.VMEM)] * n + [anywhere],
        out_specs=anywhere,
        out_shape=jax.ShapeDtypeStruct(out.shape, out.dtype),
        input_output_aliases={1 + n: 0},
        scratch_shapes=[pltpu.SemaphoreType.DMA((n,))],
        compiler_params=pltpu.CompilerParams(vmem_limit_bytes=16 * 2**20),
        cost_estimate=pl.CostEstimate(flops=3 * size, bytes_accessed=12 * size, transcendentals=0),
        name="place",
    )(me, *pieces, out)


def solution(mesh):
    def inner(*arrays):
        terms, weights, m, v = (arrays[i : i + 3] for i in (0, 3, 6, 9))
        me = lax.axis_index("dp").astype(jnp.int32).reshape(1)

        def send(x, to):
            return lax.ppermute(x, "dp", to)

        arrived, near = [], []
        for c in range(len(CHUNKS)):
            both, *more = pair(terms, c, () if c == 1 else (0, 1, 2) if c == 2 else (c,)) if c else (first_pair(terms),)
            near += more
            arrived.append(send(both, ACROSS))

        state = [() for _ in weights]
        across, beside, corner = [], [], []
        for c, (which, layer, first, rows) in enumerate(CHUNKS):
            one, *state[which] = adamw(
                me, terms[which], near[c], arrived[c], weights[which], m[which], v[which], layer, first, rows, tuple(state[which]))
            across.append(send(one, ACROSS))
            beside.append(send(one, BESIDE))
        for c in range(len(CHUNKS)):
            corner.append(send(across[c], BESIDE))
        for c in range(LAST):
            which = CHUNKS[c][0]
            together = (c,) if c < LAST - 1 else (c, LAST)
            pieces = [got[i] for i in together for got in (beside, across, corner)]
            state[which][0] = place(me, [CHUNKS[i] for i in together], pieces, state[which][0], m[which].shape[1])
        return tuple(state[which][i] for i in range(3) for which in range(3))

    all_of, cut_rows = P(None, None, None), P(None, "dp", None)
    return jax.shard_map(
        inner,
        mesh=mesh,
        in_specs=(P(("rep", "dp"), None, None, None),) * 3 + (all_of,) * 3 + (cut_rows,) * 6,
        out_specs=(P("rep", None, None),) * 3 + (P("rep", "dp", None),) * 6,
        check_vma=False,
    )
```

```python
import functools
import math

import jax
import jax.numpy as jnp
from jax import lax
from jax.experimental import pallas as pl
from jax.experimental.pallas import tpu as pltpu
from jax.sharding import PartitionSpec as P


ACROSS = [(0, 2), (2, 0), (1, 3), (3, 1)]
BESIDE = [(0, 1), (1, 0), (2, 3), (3, 2)]

CHUNKS = (
    (0, 0, 0, 48), (0, 0, 48, 80), (0, 0, 128, 128), (0, 1, 0, 256),
    (1, 0, 0, 256), (1, 1, 0, 256),
    (2, 0, 0, 768), (2, 1, 0, 384), (2, 1, 384, 240), (2, 1, 624, 96), (2, 1, 720, 48),
)
LAST = len(CHUNKS) - 1
MESH = pl.DeviceIdType.MESH


def pair_body(chunk, nears, *refs):
    n = len(nears)
    terms, (both, *near_refs) = refs[:3], refs[3 : 4 + n]
    got, mine, total, got_send, got_recv, in_sem, out_sem, near_send, near_recv = refs[4 + n :]
    which, layer, first, rows = chunk
    me = lax.axis_index("dp")
    partner = {"dp": me ^ 1}
    barrier = pltpu.get_barrier_semaphore()
    pl.semaphore_signal(barrier, inc=1, device_id=partner, device_id_type=MESH)

    def block(which, layer, first, rows, owner):
        size = terms[which].shape[2] // 4
        return terms[which].at[0, layer, pl.ds(pl.multiple_of(owner * size + first, 16), rows)]

    tile = pair_tile(rows, terms[which].shape[3])
    count = rows // tile
    owns = [
        pltpu.make_async_copy(block(which, layer, first + t * tile, tile, me ^ 2), mine.at[pl.ds(t * tile, tile)], in_sem.at[t])
        for t in range(count)
    ]
    fars = [
        pltpu.make_async_remote_copy(
            block(which, layer, first + t * tile, tile, me ^ 3), got.at[pl.ds(t * tile, tile)],
            got_send.at[t], got_recv.at[t], device_id=partner, device_id_type=MESH)
        for t in range(count)
    ]
    beside = [
        pltpu.make_async_remote_copy(
            block(*CHUNKS[c], me ^ 1), near_refs[i], near_send.at[i], near_recv.at[i], device_id=partner, device_id_type=MESH)
        for i, c in enumerate(nears)
    ]
    outs = [pltpu.make_async_copy(total.at[pl.ds(t * tile, tile)], both.at[pl.ds(t * tile, tile)], out_sem.at[t]) for t in range(count)]
    pl.semaphore_wait(barrier, 1)
    for far, own in zip(fars, owns):
        far.start()
        own.start()
    for copy in beside:
        copy.start()
    for t in range(count):
        owns[t].wait()
        fars[t].wait_recv()
        here = pl.ds(t * tile, tile)
        total[here] = (got[here].astype(jnp.float32) + mine[here].astype(jnp.float32)).astype(jnp.bfloat16)
        outs[t].start()
    for t in range(count):
        fars[t].wait_send()
        outs[t].wait()
    for copy in beside:
        copy.wait()


def first_pair_body(chunk, terms, both, got, mine, send_sem, recv_sem, in_sem):
    _, layer, first, rows = chunk
    me = lax.axis_index("dp")
    partner = {"dp": me ^ 1}
    barrier = pltpu.get_barrier_semaphore()
    pl.semaphore_signal(barrier, inc=1, device_id=partner, device_id_type=MESH)

    def block(owner):
        size = terms.shape[2] // 4
        return terms.at[0, layer, pl.ds(pl.multiple_of(owner * size + first, 16), rows)]

    own = pltpu.make_async_copy(block(me ^ 2), mine, in_sem)
    far = pltpu.make_async_remote_copy(block(me ^ 3), got, send_sem, recv_sem, device_id=partner, device_id_type=MESH)
    own.start()
    pl.semaphore_wait(barrier, 1)
    far.start()
    own.wait()
    far.wait_recv()
    both[...] = (got[...].astype(jnp.float32) + mine[...].astype(jnp.float32)).astype(jnp.bfloat16)
    far.wait_send()


def first_pair(terms):
    which, _, _, rows = CHUNKS[0]
    cols = terms[which].shape[3]
    return pl.pallas_call(
        functools.partial(first_pair_body, CHUNKS[0]),
        in_specs=[pl.BlockSpec(memory_space=pltpu.HBM)],
        out_specs=pl.BlockSpec(memory_space=pltpu.VMEM),
        out_shape=jax.ShapeDtypeStruct((rows, cols), jnp.bfloat16),
        scratch_shapes=[pltpu.VMEM((rows, cols), jnp.bfloat16)] * 2 + [pltpu.SemaphoreType.DMA] * 3,
        compiler_params=pltpu.CompilerParams(collective_id=0, has_side_effects=True, vmem_limit_bytes=52 * 2**20),
        cost_estimate=pl.CostEstimate(flops=rows * cols, bytes_accessed=8 * rows * cols, transcendentals=0),
        name="first_pair",
    )(terms[which])


def pair_tile(rows, cols):
    return math.gcd(rows, 32 * 3072 // cols)


def pair(terms, index, nears):
    chunk = CHUNKS[index]
    which, _, _, rows = chunk
    cols = terms[which].shape[3]
    count = rows // pair_tile(rows, cols)
    anywhere = pl.BlockSpec(memory_space=pl.ANY)
    shapes = [(rows, cols)] + [(CHUNKS[c][3], terms[CHUNKS[c][0]].shape[3]) for c in nears]
    return pl.pallas_call(
        functools.partial(pair_body, chunk, nears),
        in_specs=[anywhere] * 3,
        out_specs=[anywhere] * len(shapes),
        out_shape=[jax.ShapeDtypeStruct(shape, jnp.bfloat16) for shape in shapes],
        scratch_shapes=[pltpu.VMEM((rows, cols), jnp.bfloat16)] * 3
        + [pltpu.SemaphoreType.DMA((count,))] * 4
        + [pltpu.SemaphoreType.DMA((max(1, len(nears)),))] * 2,
        compiler_params=pltpu.CompilerParams(collective_id=index, has_side_effects=True),
        cost_estimate=pl.CostEstimate(flops=rows * cols, bytes_accessed=10 * rows * cols, transcendentals=0),
        name="pair",
    )(*terms)


def adamw_body(n_alias, me, own, near, far, w, m, v, *rest):
    send, out, m_out, v_out = rest[n_alias:]
    g = own[...].astype(jnp.float32) + near[...].astype(jnp.float32) + far[...].astype(jnp.float32)
    g = g.reshape(m.shape).astype(jnp.bfloat16).astype(jnp.float32)
    m_new = 0.9 * m[...] + 0.1 * g
    v_new = 0.95 * v[...] + 0.05 * g * g
    w_old = w[...].astype(jnp.float32)
    new = (w_old - 0.02 * (m_new * lax.rsqrt(v_new + 1e-8) + 0.1 * w_old)).astype(jnp.bfloat16)
    send[...] = new.reshape(send.shape)
    out[...] = new
    m_out[...] = m_new
    v_out[...] = v_new


def adamw(me, terms, near, far, w, m, v, layer, first, rows, before):
    block, cols = m.shape[1], m.shape[2]
    tile = math.gcd(rows, first, block, 32 * 3072 // cols)
    at, per = first // tile, block // tile
    mine = pl.BlockSpec((1, tile, cols), lambda i, me: (layer, at + i, 0))
    whole = pl.BlockSpec((1, tile, cols), lambda i, me: (layer, me[0] * per + at + i, 0))
    term = pl.BlockSpec((1, 1, tile, cols), lambda i, me: (0, layer, me[0] * per + at + i, 0))
    chunk = pl.BlockSpec((tile, cols), lambda i, me: (i, 0))
    anywhere = pl.BlockSpec(memory_space=pl.ANY)
    n_alias = len(before)
    size = rows * cols
    return pl.pallas_call(
        functools.partial(adamw_body, n_alias),
        grid_spec=pltpu.PrefetchScalarGridSpec(
            num_scalar_prefetch=1,
            grid=(rows // tile,),
            in_specs=[term, chunk, chunk, whole, mine, mine] + [anywhere] * n_alias,
            out_specs=[chunk, whole, mine, mine],
        ),
        out_shape=[
            jax.ShapeDtypeStruct((rows, cols), jnp.bfloat16),
            jax.ShapeDtypeStruct(w.shape, jnp.bfloat16),
            jax.ShapeDtypeStruct(m.shape, jnp.float32),
            jax.ShapeDtypeStruct(v.shape, jnp.float32),
        ],
        input_output_aliases={7 + i: 1 + i for i in range(n_alias)},
        cost_estimate=pl.CostEstimate(flops=14 * size, bytes_accessed=28 * size, transcendentals=size),
        name="adamw",
    )(me, terms, near, far, w, m, v, *before)


def place_body(chunks, block, me, *refs):
    pieces, (_, out, sem) = refs[: 3 * len(chunks)], refs[3 * len(chunks) :]
    copies = []
    for i, src in enumerate(pieces):
        _, layer, first, rows = chunks[i // 3]
        owner = me[0] ^ (1 + i % 3)
        copies.append(pltpu.make_async_copy(src, out.at[layer, pl.ds(pl.multiple_of(owner * block + first, 16), rows)], sem.at[i]))
    for copy in copies:
        copy.start()
    for copy in copies:
        copy.wait()


def place(me, chunks, pieces, out, block):
    cols = out.shape[2]
    size = sum(chunk[3] for chunk in chunks) * cols
    anywhere = pl.BlockSpec(memory_space=pl.ANY)
    n = 3 * len(chunks)
    return pl.pallas_call(
        functools.partial(place_body, chunks, block),
        in_specs=[pl.BlockSpec(memory_space=pltpu.SMEM)] + [pl.BlockSpec(memory_space=pltpu.VMEM)] * n + [anywhere],
        out_specs=anywhere,
        out_shape=jax.ShapeDtypeStruct(out.shape, out.dtype),
        input_output_aliases={1 + n: 0},
        scratch_shapes=[pltpu.SemaphoreType.DMA((n,))],
        compiler_params=pltpu.CompilerParams(vmem_limit_bytes=16 * 2**20),
        cost_estimate=pl.CostEstimate(flops=3 * size, bytes_accessed=12 * size, transcendentals=0),
        name="place",
    )(me, *pieces, out)


def carry_body(chunk, block, me, beside, across, corner, before, out, held, in_sem, out_sem):
    _, layer, first, rows = chunk
    ins = [pltpu.make_async_copy(src, held.at[i], in_sem.at[i]) for i, src in enumerate((beside, across, corner))]
    outs = [
        pltpu.make_async_copy(held.at[i], out.at[layer, pl.ds(pl.multiple_of((me[0] ^ (1 + i)) * block + first, 16), rows)], out_sem.at[i])
        for i in range(3)
    ]
    for copy in ins:
        copy.start()
    for came, goes in zip(ins, outs):
        came.wait()
        goes.start()
    for copy in outs:
        copy.wait()


def carry(me, chunk, pieces, out, block):
    _, _, _, rows = chunk
    cols = out.shape[2]
    anywhere = pl.BlockSpec(memory_space=pl.ANY)
    return pl.pallas_call(
        functools.partial(carry_body, chunk, block),
        in_specs=[pl.BlockSpec(memory_space=pltpu.SMEM)] + [anywhere] * 4,
        out_specs=anywhere,
        out_shape=jax.ShapeDtypeStruct(out.shape, out.dtype),
        input_output_aliases={4: 0},
        scratch_shapes=[
            pltpu.VMEM((3, rows, cols), jnp.bfloat16),
            pltpu.SemaphoreType.DMA((3,)),
            pltpu.SemaphoreType.DMA((3,)),
        ],
        cost_estimate=pl.CostEstimate(flops=3 * rows * cols, bytes_accessed=12 * rows * cols, transcendentals=0),
        name="carry",
    )(me, *pieces, out)


def solution(mesh):
    def inner(*arrays):
        terms, weights, m, v = (arrays[i : i + 3] for i in (0, 3, 6, 9))
        me = lax.axis_index("dp").astype(jnp.int32).reshape(1)

        def send(x, to):
            return lax.ppermute(x, "dp", to)

        arrived, near = [], []
        for c in range(len(CHUNKS)):
            both, *more = pair(terms, c, () if c == 1 else (0, 1, 2) if c == 2 else (c,)) if c else (first_pair(terms),)
            near += more
            arrived.append(send(both, ACROSS))

        state = [() for _ in weights]
        across, beside, corner = [], [], []
        for c, (which, layer, first, rows) in enumerate(CHUNKS):
            one, *state[which] = adamw(
                me, terms[which], near[c], arrived[c], weights[which], m[which], v[which], layer, first, rows, tuple(state[which]))
            across.append(send(one, ACROSS))
            beside.append(send(one, BESIDE))
        for c in range(len(CHUNKS)):
            corner.append(send(across[c], BESIDE))
        for c in range(LAST):
            which = CHUNKS[c][0]
            together = (c,) if c < LAST - 1 else (c, LAST)
            pieces = [got[i] for i in together for got in (beside, across, corner)]
            if c < LAST - 2:
                state[which][0] = carry(me, CHUNKS[c], pieces, state[which][0], m[which].shape[1])
            else:
                state[which][0] = place(me, [CHUNKS[i] for i in together], pieces, state[which][0], m[which].shape[1])
        return tuple(state[which][i] for i in range(3) for which in range(3))

    all_of, cut_rows = P(None, None, None), P(None, "dp", None)
    return jax.shard_map(
        inner,
        mesh=mesh,
        in_specs=(P(("rep", "dp"), None, None, None),) * 3 + (all_of,) * 3 + (cut_rows,) * 6,
        out_specs=(P("rep", None, None),) * 3 + (P("rep", "dp", None),) * 6,
        check_vma=False,
    )
```

```python
import functools
import math

import jax
import jax.numpy as jnp
from jax import lax
from jax.experimental import pallas as pl
from jax.experimental.pallas import tpu as pltpu
from jax.sharding import PartitionSpec as P


ACROSS = [(0, 2), (2, 0), (1, 3), (3, 1)]
BESIDE = [(0, 1), (1, 0), (2, 3), (3, 2)]

CHUNKS = (
    (0, 0, 0, 48), (0, 0, 48, 80), (0, 0, 128, 128), (0, 1, 0, 256),
    (1, 0, 0, 256), (1, 1, 0, 256),
    (2, 0, 0, 768), (2, 1, 0, 384), (2, 1, 384, 240), (2, 1, 624, 96), (2, 1, 720, 48),
)
LAST = len(CHUNKS) - 1
MESH = pl.DeviceIdType.MESH


def pair_body(chunk, nears, *refs):
    n = len(nears)
    terms, (both, *near_refs) = refs[:3], refs[3 : 4 + n]
    got, mine, total, got_send, got_recv, in_sem, out_sem, near_send, near_recv = refs[4 + n :]
    which, layer, first, rows = chunk
    me = lax.axis_index("dp")
    partner = {"dp": me ^ 1}
    barrier = pltpu.get_barrier_semaphore()
    pl.semaphore_signal(barrier, inc=1, device_id=partner, device_id_type=MESH)

    def block(which, layer, first, rows, owner):
        size = terms[which].shape[2] // 4
        return terms[which].at[0, layer, pl.ds(pl.multiple_of(owner * size + first, 16), rows)]

    tile = pair_tile(rows, terms[which].shape[3])
    count = rows // tile
    owns = [
        pltpu.make_async_copy(block(which, layer, first + t * tile, tile, me ^ 2), mine.at[pl.ds(t * tile, tile)], in_sem.at[t])
        for t in range(count)
    ]
    fars = [
        pltpu.make_async_remote_copy(
            block(which, layer, first + t * tile, tile, me ^ 3), got.at[pl.ds(t * tile, tile)],
            got_send.at[t], got_recv.at[t], device_id=partner, device_id_type=MESH)
        for t in range(count)
    ]
    beside = [
        pltpu.make_async_remote_copy(
            block(*CHUNKS[c], me ^ 1), near_refs[i], near_send.at[i], near_recv.at[i], device_id=partner, device_id_type=MESH)
        for i, c in enumerate(nears)
    ]
    outs = [pltpu.make_async_copy(total.at[pl.ds(t * tile, tile)], both.at[pl.ds(t * tile, tile)], out_sem.at[t]) for t in range(count)]
    pl.semaphore_wait(barrier, 1)
    for far, own in zip(fars, owns):
        far.start()
        own.start()
    for copy in beside:
        copy.start()
    for t in range(count):
        owns[t].wait()
        fars[t].wait_recv()
        here = pl.ds(t * tile, tile)
        total[here] = (got[here].astype(jnp.float32) + mine[here].astype(jnp.float32)).astype(jnp.bfloat16)
        outs[t].start()
    for t in range(count):
        fars[t].wait_send()
        outs[t].wait()
    for copy in beside:
        copy.wait()


def first_pair_body(chunk, terms, both, got, mine, send_sem, recv_sem, in_sem):
    _, layer, first, rows = chunk
    me = lax.axis_index("dp")
    partner = {"dp": me ^ 1}
    barrier = pltpu.get_barrier_semaphore()
    pl.semaphore_signal(barrier, inc=1, device_id=partner, device_id_type=MESH)

    def block(owner):
        size = terms.shape[2] // 4
        return terms.at[0, layer, pl.ds(pl.multiple_of(owner * size + first, 16), rows)]

    own = pltpu.make_async_copy(block(me ^ 2), mine, in_sem)
    far = pltpu.make_async_remote_copy(block(me ^ 3), got, send_sem, recv_sem, device_id=partner, device_id_type=MESH)
    own.start()
    pl.semaphore_wait(barrier, 1)
    far.start()
    own.wait()
    far.wait_recv()
    both[...] = (got[...].astype(jnp.float32) + mine[...].astype(jnp.float32)).astype(jnp.bfloat16)
    far.wait_send()


def first_pair(terms):
    which, _, _, rows = CHUNKS[0]
    cols = terms[which].shape[3]
    return pl.pallas_call(
        functools.partial(first_pair_body, CHUNKS[0]),
        in_specs=[pl.BlockSpec(memory_space=pltpu.HBM)],
        out_specs=pl.BlockSpec(memory_space=pltpu.VMEM),
        out_shape=jax.ShapeDtypeStruct((rows, cols), jnp.bfloat16),
        scratch_shapes=[pltpu.VMEM((rows, cols), jnp.bfloat16)] * 2 + [pltpu.SemaphoreType.DMA] * 3,
        compiler_params=pltpu.CompilerParams(collective_id=0, has_side_effects=True, vmem_limit_bytes=52 * 2**20),
        cost_estimate=pl.CostEstimate(flops=rows * cols, bytes_accessed=8 * rows * cols, transcendentals=0),
        name="first_pair",
    )(terms[which])


def pair_tile(rows, cols):
    return rows if rows * cols <= 96 * 3072 else math.gcd(rows, 64 * 3072 // cols)


def pair(terms, index, nears):
    chunk = CHUNKS[index]
    which, _, _, rows = chunk
    cols = terms[which].shape[3]
    count = rows // pair_tile(rows, cols)
    anywhere = pl.BlockSpec(memory_space=pl.ANY)
    shapes = [(rows, cols)] + [(CHUNKS[c][3], terms[CHUNKS[c][0]].shape[3]) for c in nears]
    return pl.pallas_call(
        functools.partial(pair_body, chunk, nears),
        in_specs=[anywhere] * 3,
        out_specs=[anywhere] * len(shapes),
        out_shape=[jax.ShapeDtypeStruct(shape, jnp.bfloat16) for shape in shapes],
        scratch_shapes=[pltpu.VMEM((rows, cols), jnp.bfloat16)] * 3
        + [pltpu.SemaphoreType.DMA((count,))] * 4
        + [pltpu.SemaphoreType.DMA((max(1, len(nears)),))] * 2,
        compiler_params=pltpu.CompilerParams(collective_id=index, has_side_effects=True),
        cost_estimate=pl.CostEstimate(flops=rows * cols, bytes_accessed=10 * rows * cols, transcendentals=0),
        name="pair",
    )(*terms)


def adamw_body(n_alias, me, own, near, far, w, m, v, *rest):
    send, out, m_out, v_out = rest[n_alias:]
    g = own[...].astype(jnp.float32) + near[...].astype(jnp.float32) + far[...].astype(jnp.float32)
    g = g.reshape(m.shape).astype(jnp.bfloat16).astype(jnp.float32)
    m_new = 0.9 * m[...] + 0.1 * g
    v_new = 0.95 * v[...] + 0.05 * g * g
    w_old = w[...].astype(jnp.float32)
    new = (w_old - 0.02 * (m_new * lax.rsqrt(v_new + 1e-8) + 0.1 * w_old)).astype(jnp.bfloat16)
    send[...] = new.reshape(send.shape)
    out[...] = new
    m_out[...] = m_new
    v_out[...] = v_new


def adamw(me, terms, near, far, w, m, v, layer, first, rows, before):
    block, cols = m.shape[1], m.shape[2]
    tile = math.gcd(rows, first, block, 64 * 3072 // cols)
    at, per = first // tile, block // tile
    mine = pl.BlockSpec((1, tile, cols), lambda i, me: (layer, at + i, 0))
    whole = pl.BlockSpec((1, tile, cols), lambda i, me: (layer, me[0] * per + at + i, 0))
    term = pl.BlockSpec((1, 1, tile, cols), lambda i, me: (0, layer, me[0] * per + at + i, 0))
    chunk = pl.BlockSpec((tile, cols), lambda i, me: (i, 0))
    anywhere = pl.BlockSpec(memory_space=pl.ANY)
    n_alias = len(before)
    size = rows * cols
    return pl.pallas_call(
        functools.partial(adamw_body, n_alias),
        grid_spec=pltpu.PrefetchScalarGridSpec(
            num_scalar_prefetch=1,
            grid=(rows // tile,),
            in_specs=[term, chunk, chunk, whole, mine, mine] + [anywhere] * n_alias,
            out_specs=[chunk, whole, mine, mine],
        ),
        out_shape=[
            jax.ShapeDtypeStruct((rows, cols), jnp.bfloat16),
            jax.ShapeDtypeStruct(w.shape, jnp.bfloat16),
            jax.ShapeDtypeStruct(m.shape, jnp.float32),
            jax.ShapeDtypeStruct(v.shape, jnp.float32),
        ],
        input_output_aliases={7 + i: 1 + i for i in range(n_alias)},
        cost_estimate=pl.CostEstimate(flops=14 * size, bytes_accessed=28 * size, transcendentals=size),
        name="adamw",
    )(me, terms, near, far, w, m, v, *before)


def place_body(what, block, me, *refs):
    pieces, (_, out, sem) = refs[:-3], refs[-3:]
    copies = []
    for i, ((c, other), src) in enumerate(zip(what, pieces, strict=True)):
        _, layer, first, rows = CHUNKS[c]
        to = out.at[layer, pl.ds(pl.multiple_of((me[0] ^ other) * block + first, 16), rows)]
        copies.append(pltpu.make_async_copy(src, to, sem.at[i]))
    for copy in copies:
        copy.start()
    for copy in copies:
        copy.wait()


def place(me, what, pieces, out, block):
    size = sum(piece.size for piece in pieces)
    anywhere = pl.BlockSpec(memory_space=pl.ANY)
    n = len(pieces)
    return pl.pallas_call(
        functools.partial(place_body, what, block),
        in_specs=[pl.BlockSpec(memory_space=pltpu.SMEM)] + [pl.BlockSpec(memory_space=pltpu.VMEM)] * n + [anywhere],
        out_specs=anywhere,
        out_shape=jax.ShapeDtypeStruct(out.shape, out.dtype),
        input_output_aliases={1 + n: 0},
        scratch_shapes=[pltpu.SemaphoreType.DMA((n,))],
        compiler_params=pltpu.CompilerParams(vmem_limit_bytes=16 * 2**20),
        cost_estimate=pl.CostEstimate(flops=size, bytes_accessed=4 * size, transcendentals=0),
        name="place",
    )(me, *pieces, out)


def carry_body(chunk, block, me, beside, across, corner, before, out, held, in_sem, out_sem):
    _, layer, first, rows = chunk
    ins = [pltpu.make_async_copy(src, held.at[i], in_sem.at[i]) for i, src in enumerate((beside, across, corner))]
    outs = [
        pltpu.make_async_copy(held.at[i], out.at[layer, pl.ds(pl.multiple_of((me[0] ^ (1 + i)) * block + first, 16), rows)], out_sem.at[i])
        for i in range(3)
    ]
    for copy in ins:
        copy.start()
    for came, goes in zip(ins, outs):
        came.wait()
        goes.start()
    for copy in outs:
        copy.wait()


def carry(me, chunk, pieces, out, block):
    _, _, _, rows = chunk
    cols = out.shape[2]
    anywhere = pl.BlockSpec(memory_space=pl.ANY)
    return pl.pallas_call(
        functools.partial(carry_body, chunk, block),
        in_specs=[pl.BlockSpec(memory_space=pltpu.SMEM)] + [anywhere] * 4,
        out_specs=anywhere,
        out_shape=jax.ShapeDtypeStruct(out.shape, out.dtype),
        input_output_aliases={4: 0},
        scratch_shapes=[
            pltpu.VMEM((3, rows, cols), jnp.bfloat16),
            pltpu.SemaphoreType.DMA((3,)),
            pltpu.SemaphoreType.DMA((3,)),
        ],
        cost_estimate=pl.CostEstimate(flops=3 * rows * cols, bytes_accessed=12 * rows * cols, transcendentals=0),
        name="carry",
    )(me, *pieces, out)


def solution(mesh):
    def inner(*arrays):
        terms, weights, m, v = (arrays[i : i + 3] for i in (0, 3, 6, 9))
        me = lax.axis_index("dp").astype(jnp.int32).reshape(1)

        def send(x, to):
            return lax.ppermute(x, "dp", to)

        arrived, near = [], []
        for c in range(len(CHUNKS)):
            both, *more = pair(terms, c, () if c == 1 else (0, 1, 2) if c == 2 else (c,)) if c else (first_pair(terms),)
            near += more
            arrived.append(send(both, ACROSS))

        state = [() for _ in weights]
        across, beside, corner = [], [], []
        for c, (which, layer, first, rows) in enumerate(CHUNKS):
            one, *state[which] = adamw(
                me, terms[which], near[c], arrived[c], weights[which], m[which], v[which], layer, first, rows, tuple(state[which]))
            across.append(send(one, ACROSS))
            beside.append(send(one, BESIDE))
        for c in range(len(CHUNKS)):
            corner.append(send(across[c], BESIDE))
        came = {1: beside, 2: across, 3: corner}
        for c in range(LAST):
            which = CHUNKS[c][0]
            what = ((c, 1), (c, 2), (c, 3))
            if c == LAST - 2:
                what += ((LAST - 1, 1), (LAST, 1))
            if c == LAST - 1:
                what = ((c, 2), (c, 3), (LAST, 2))
            pieces = [came[other][i] for i, other in what]
            if c < LAST - 2:
                state[which][0] = carry(me, CHUNKS[c], pieces, state[which][0], m[which].shape[1])
            else:
                state[which][0] = place(me, what, pieces, state[which][0], m[which].shape[1])
        which, layer, first, _ = CHUNKS[LAST]
        row = (lax.axis_index("dp") ^ 3) * m[which].shape[1] + first
        state[which][0] = lax.dynamic_update_slice(state[which][0], corner[LAST][None], (layer, row, 0))
        return tuple(state[which][i] for i in range(3) for which in range(3))

    all_of, cut_rows = P(None, None, None), P(None, "dp", None)
    return jax.shard_map(
        inner,
        mesh=mesh,
        in_specs=(P(("rep", "dp"), None, None, None),) * 3 + (all_of,) * 3 + (cut_rows,) * 6,
        out_specs=(P("rep", None, None),) * 3 + (P("rep", "dp", None),) * 6,
        check_vma=False,
    )
```

```python
import functools
import math

import jax
import jax.numpy as jnp
from jax import lax
from jax.experimental import pallas as pl
from jax.experimental.pallas import tpu as pltpu
from jax.sharding import PartitionSpec as P


ACROSS = [(0, 2), (2, 0), (1, 3), (3, 1)]
BESIDE = [(0, 1), (1, 0), (2, 3), (3, 2)]

CHUNKS = (
    (0, 0, 0, 32), (0, 0, 32, 32), (0, 0, 64, 64), (0, 0, 128, 128), (0, 1, 0, 256),
    (1, 0, 0, 256), (1, 1, 0, 256),
    (2, 0, 0, 768), (2, 1, 0, 384), (2, 1, 384, 192), (2, 1, 576, 96), (2, 1, 672, 48), (2, 1, 720, 48),
)
LAST = len(CHUNKS) - 1
MESH = pl.DeviceIdType.MESH


def pair_body(chunk, nears, *refs):
    n = len(nears)
    terms, (both, *near_refs) = refs[:3], refs[3 : 4 + n]
    got, mine, total, got_send, got_recv, in_sem, out_sem, near_send, near_recv = refs[4 + n :]
    which, layer, first, rows = chunk
    me = lax.axis_index("dp")
    partner = {"dp": me ^ 1}
    barrier = pltpu.get_barrier_semaphore()
    pl.semaphore_signal(barrier, inc=1, device_id=partner, device_id_type=MESH)

    def block(which, layer, first, rows, owner):
        size = terms[which].shape[2] // 4
        return terms[which].at[0, layer, pl.ds(pl.multiple_of(owner * size + first, 16), rows)]

    tile = pair_tile(rows, terms[which].shape[3])
    count = rows // tile
    owns = [
        pltpu.make_async_copy(block(which, layer, first + t * tile, tile, me ^ 2), mine.at[pl.ds(t * tile, tile)], in_sem.at[t])
        for t in range(count)
    ]
    fars = [
        pltpu.make_async_remote_copy(
            block(which, layer, first + t * tile, tile, me ^ 3), got.at[pl.ds(t * tile, tile)],
            got_send.at[t], got_recv.at[t], device_id=partner, device_id_type=MESH)
        for t in range(count)
    ]
    beside = [
        pltpu.make_async_remote_copy(
            block(*CHUNKS[c], me ^ 1), near_refs[i], near_send.at[i], near_recv.at[i], device_id=partner, device_id_type=MESH)
        for i, c in enumerate(nears)
    ]
    outs = [pltpu.make_async_copy(total.at[pl.ds(t * tile, tile)], both.at[pl.ds(t * tile, tile)], out_sem.at[t]) for t in range(count)]
    pl.semaphore_wait(barrier, 1)
    for far, own in zip(fars, owns):
        far.start()
        own.start()
    for copy in beside:
        copy.start()
    for t in range(count):
        owns[t].wait()
        fars[t].wait_recv()
        here = pl.ds(t * tile, tile)
        total[here] = (got[here].astype(jnp.float32) + mine[here].astype(jnp.float32)).astype(jnp.bfloat16)
        outs[t].start()
    for t in range(count):
        fars[t].wait_send()
        outs[t].wait()
    for copy in beside:
        copy.wait()


def first_pair_body(chunk, terms, both, got, mine, send_sem, recv_sem, in_sem):
    _, layer, first, rows = chunk
    me = lax.axis_index("dp")
    partner = {"dp": me ^ 1}
    barrier = pltpu.get_barrier_semaphore()
    pl.semaphore_signal(barrier, inc=1, device_id=partner, device_id_type=MESH)

    def block(owner):
        size = terms.shape[2] // 4
        return terms.at[0, layer, pl.ds(pl.multiple_of(owner * size + first, 16), rows)]

    own = pltpu.make_async_copy(block(me ^ 2), mine, in_sem)
    far = pltpu.make_async_remote_copy(block(me ^ 3), got, send_sem, recv_sem, device_id=partner, device_id_type=MESH)
    own.start()
    pl.semaphore_wait(barrier, 1)
    far.start()
    own.wait()
    far.wait_recv()
    both[...] = (got[...].astype(jnp.float32) + mine[...].astype(jnp.float32)).astype(jnp.bfloat16)
    far.wait_send()


def first_pair(terms):
    which, _, _, rows = CHUNKS[0]
    cols = terms[which].shape[3]
    return pl.pallas_call(
        functools.partial(first_pair_body, CHUNKS[0]),
        in_specs=[pl.BlockSpec(memory_space=pltpu.HBM)],
        out_specs=pl.BlockSpec(memory_space=pltpu.VMEM),
        out_shape=jax.ShapeDtypeStruct((rows, cols), jnp.bfloat16),
        scratch_shapes=[pltpu.VMEM((rows, cols), jnp.bfloat16)] * 2 + [pltpu.SemaphoreType.DMA] * 3,
        compiler_params=pltpu.CompilerParams(collective_id=0, has_side_effects=True, vmem_limit_bytes=52 * 2**20),
        cost_estimate=pl.CostEstimate(flops=rows * cols, bytes_accessed=8 * rows * cols, transcendentals=0),
        name="first_pair",
    )(terms[which])


def pair_tile(rows, cols):
    return rows if rows * cols <= 96 * 3072 else math.gcd(rows, 64 * 3072 // cols)


def pair(terms, index, nears):
    chunk = CHUNKS[index]
    which, _, _, rows = chunk
    cols = terms[which].shape[3]
    count = rows // pair_tile(rows, cols)
    anywhere = pl.BlockSpec(memory_space=pl.ANY)
    shapes = [(rows, cols)] + [(CHUNKS[c][3], terms[CHUNKS[c][0]].shape[3]) for c in nears]
    return pl.pallas_call(
        functools.partial(pair_body, chunk, nears),
        in_specs=[anywhere] * 3,
        out_specs=[anywhere] * len(shapes),
        out_shape=[jax.ShapeDtypeStruct(shape, jnp.bfloat16) for shape in shapes],
        scratch_shapes=[pltpu.VMEM((rows, cols), jnp.bfloat16)] * 3
        + [pltpu.SemaphoreType.DMA((count,))] * 4
        + [pltpu.SemaphoreType.DMA((max(1, len(nears)),))] * 2,
        compiler_params=pltpu.CompilerParams(collective_id=index, has_side_effects=True),
        cost_estimate=pl.CostEstimate(flops=rows * cols, bytes_accessed=10 * rows * cols, transcendentals=0),
        name="pair",
    )(*terms)


def adamw_body(n_alias, me, own, near, far, w, m, v, *rest):
    send, out, m_out, v_out = rest[n_alias:]
    g = own[...].astype(jnp.float32) + near[...].astype(jnp.float32) + far[...].astype(jnp.float32)
    g = g.reshape(m.shape).astype(jnp.bfloat16).astype(jnp.float32)
    m_new = 0.9 * m[...] + 0.1 * g
    v_new = 0.95 * v[...] + 0.05 * g * g
    w_old = w[...].astype(jnp.float32)
    new = (w_old - 0.02 * (m_new * lax.rsqrt(v_new + 1e-8) + 0.1 * w_old)).astype(jnp.bfloat16)
    send[...] = new.reshape(send.shape)
    out[...] = new
    m_out[...] = m_new
    v_out[...] = v_new


def adamw(me, terms, near, far, w, m, v, layer, first, rows, before):
    block, cols = m.shape[1], m.shape[2]
    tile = math.gcd(rows, first, block, 64 * 3072 // cols)
    at, per = first // tile, block // tile
    mine = pl.BlockSpec((1, tile, cols), lambda i, me: (layer, at + i, 0))
    whole = pl.BlockSpec((1, tile, cols), lambda i, me: (layer, me[0] * per + at + i, 0))
    term = pl.BlockSpec((1, 1, tile, cols), lambda i, me: (0, layer, me[0] * per + at + i, 0))
    chunk = pl.BlockSpec((tile, cols), lambda i, me: (i, 0))
    anywhere = pl.BlockSpec(memory_space=pl.ANY)
    n_alias = len(before)
    size = rows * cols
    return pl.pallas_call(
        functools.partial(adamw_body, n_alias),
        grid_spec=pltpu.PrefetchScalarGridSpec(
            num_scalar_prefetch=1,
            grid=(rows // tile,),
            in_specs=[term, chunk, chunk, whole, mine, mine] + [anywhere] * n_alias,
            out_specs=[chunk, whole, mine, mine],
        ),
        out_shape=[
            jax.ShapeDtypeStruct((rows, cols), jnp.bfloat16),
            jax.ShapeDtypeStruct(w.shape, jnp.bfloat16),
            jax.ShapeDtypeStruct(m.shape, jnp.float32),
            jax.ShapeDtypeStruct(v.shape, jnp.float32),
        ],
        input_output_aliases={7 + i: 1 + i for i in range(n_alias)},
        cost_estimate=pl.CostEstimate(flops=14 * size, bytes_accessed=28 * size, transcendentals=size),
        name="adamw",
    )(me, terms, near, far, w, m, v, *before)


def place_body(what, block, me, *refs):
    pieces, (_, out, sem) = refs[:-3], refs[-3:]
    copies = []
    for i, ((c, other), src) in enumerate(zip(what, pieces, strict=True)):
        _, layer, first, rows = CHUNKS[c]
        to = out.at[layer, pl.ds(pl.multiple_of((me[0] ^ other) * block + first, 16), rows)]
        copies.append(pltpu.make_async_copy(src, to, sem.at[i]))
    for copy in copies:
        copy.start()
    for copy in copies:
        copy.wait()


def place(me, what, pieces, out, block):
    size = sum(piece.size for piece in pieces)
    anywhere = pl.BlockSpec(memory_space=pl.ANY)
    n = len(pieces)
    return pl.pallas_call(
        functools.partial(place_body, what, block),
        in_specs=[pl.BlockSpec(memory_space=pltpu.SMEM)] + [pl.BlockSpec(memory_space=pltpu.VMEM)] * n + [anywhere],
        out_specs=anywhere,
        out_shape=jax.ShapeDtypeStruct(out.shape, out.dtype),
        input_output_aliases={1 + n: 0},
        scratch_shapes=[pltpu.SemaphoreType.DMA((n,))],
        compiler_params=pltpu.CompilerParams(vmem_limit_bytes=16 * 2**20),
        cost_estimate=pl.CostEstimate(flops=size, bytes_accessed=4 * size, transcendentals=0),
        name="place",
    )(me, *pieces, out)


def carry_body(chunk, block, me, beside, across, corner, before, out, held, in_sem, out_sem):
    _, layer, first, rows = chunk
    ins = [pltpu.make_async_copy(src, held.at[i], in_sem.at[i]) for i, src in enumerate((beside, across, corner))]
    outs = [
        pltpu.make_async_copy(held.at[i], out.at[layer, pl.ds(pl.multiple_of((me[0] ^ (1 + i)) * block + first, 16), rows)], out_sem.at[i])
        for i in range(3)
    ]
    for copy in ins:
        copy.start()
    for came, goes in zip(ins, outs):
        came.wait()
        goes.start()
    for copy in outs:
        copy.wait()


def carry(me, chunk, pieces, out, block):
    _, _, _, rows = chunk
    cols = out.shape[2]
    anywhere = pl.BlockSpec(memory_space=pl.ANY)
    return pl.pallas_call(
        functools.partial(carry_body, chunk, block),
        in_specs=[pl.BlockSpec(memory_space=pltpu.SMEM)] + [anywhere] * 4,
        out_specs=anywhere,
        out_shape=jax.ShapeDtypeStruct(out.shape, out.dtype),
        input_output_aliases={4: 0},
        scratch_shapes=[
            pltpu.VMEM((3, rows, cols), jnp.bfloat16),
            pltpu.SemaphoreType.DMA((3,)),
            pltpu.SemaphoreType.DMA((3,)),
        ],
        cost_estimate=pl.CostEstimate(flops=3 * rows * cols, bytes_accessed=12 * rows * cols, transcendentals=0),
        name="carry",
    )(me, *pieces, out)


def solution(mesh):
    def inner(*arrays):
        terms, weights, m, v = (arrays[i : i + 3] for i in (0, 3, 6, 9))
        me = lax.axis_index("dp").astype(jnp.int32).reshape(1)

        def send(x, to):
            return lax.ppermute(x, "dp", to)

        arrived, near = [], []
        for c in range(len(CHUNKS)):
            both, *more = pair(terms, c, () if c < 3 else (0, 1, 2, 3) if c == 3 else (c,)) if c else (first_pair(terms),)
            near += more
            arrived.append(send(both, ACROSS))

        state = [() for _ in weights]
        across, beside, corner = [], [], []
        for c, (which, layer, first, rows) in enumerate(CHUNKS):
            one, *state[which] = adamw(
                me, terms[which], near[c], arrived[c], weights[which], m[which], v[which], layer, first, rows, tuple(state[which]))
            across.append(send(one, ACROSS))
            beside.append(send(one, BESIDE))
        for c in range(len(CHUNKS)):
            corner.append(send(across[c], BESIDE))
        came = {1: beside, 2: across, 3: corner}
        for c in range(LAST):
            which = CHUNKS[c][0]
            what = ((c, 1), (c, 2), (c, 3))
            if c == LAST - 2:
                what += ((LAST - 1, 1), (LAST, 1))
            if c == LAST - 1:
                what = ((c, 2), (c, 3), (LAST, 2))
            pieces = [came[other][i] for i, other in what]
            if c < LAST - 2:
                state[which][0] = carry(me, CHUNKS[c], pieces, state[which][0], m[which].shape[1])
            else:
                state[which][0] = place(me, what, pieces, state[which][0], m[which].shape[1])
        which, layer, first, _ = CHUNKS[LAST]
        row = (lax.axis_index("dp") ^ 3) * m[which].shape[1] + first
        state[which][0] = lax.dynamic_update_slice(state[which][0], corner[LAST][None], (layer, row, 0))
        return tuple(state[which][i] for i in range(3) for which in range(3))

    all_of, cut_rows = P(None, None, None), P(None, "dp", None)
    return jax.shard_map(
        inner,
        mesh=mesh,
        in_specs=(P(("rep", "dp"), None, None, None),) * 3 + (all_of,) * 3 + (cut_rows,) * 6,
        out_specs=(P("rep", None, None),) * 3 + (P("rep", "dp", None),) * 6,
        check_vma=False,
    )
```

```python
import functools
import math

import jax
import jax.numpy as jnp
from jax import lax
from jax.experimental import pallas as pl
from jax.experimental.pallas import tpu as pltpu
from jax.sharding import PartitionSpec as P


ACROSS = [(0, 2), (2, 0), (1, 3), (3, 1)]
BESIDE = [(0, 1), (1, 0), (2, 3), (3, 2)]

SUMS = (
    (0, 0, 0, 32), (0, 0, 32, 32), (0, 0, 64, 64), (0, 0, 128, 128), (0, 1, 0, 256),
    (1, 0, 0, 256), (1, 1, 0, 256), (2, 0, 0, 768), (2, 1, 0, 768),
)
CHUNKS = (
    (0, 0, 0, 256), (0, 1, 0, 256), (1, 0, 0, 256), (1, 1, 0, 256),
    (2, 0, 0, 768), (2, 1, 0, 384), (2, 1, 384, 192), (2, 1, 576, 96), (2, 1, 672, 48), (2, 1, 720, 48),
)
STEPS = tuple(
    (r, c, max(sums[2], chunk[2]), min(sums[3], chunk[3]))
    for r, sums in enumerate(SUMS)
    for c, chunk in enumerate(CHUNKS)
    if sums[:2] == chunk[:2] and sums[2] < chunk[2] + chunk[3] and chunk[2] < sums[2] + sums[3]
)
LAST = len(CHUNKS) - 1
MESH = pl.DeviceIdType.MESH


def pair_body(chunk, nears, *refs):
    n = len(nears)
    terms, (both, *near_refs) = refs[:3], refs[3 : 4 + n]
    got, mine, total, got_send, got_recv, in_sem, out_sem, near_send, near_recv = refs[4 + n :]
    which, layer, first, rows = chunk
    me = lax.axis_index("dp")
    partner = {"dp": me ^ 1}
    barrier = pltpu.get_barrier_semaphore()
    pl.semaphore_signal(barrier, inc=1, device_id=partner, device_id_type=MESH)

    def block(which, layer, first, rows, owner):
        size = terms[which].shape[2] // 4
        return terms[which].at[0, layer, pl.ds(pl.multiple_of(owner * size + first, 16), rows)]

    tile = pair_tile(rows, terms[which].shape[3])
    count = rows // tile
    owns = [
        pltpu.make_async_copy(block(which, layer, first + t * tile, tile, me ^ 2), mine.at[pl.ds(t * tile, tile)], in_sem.at[t])
        for t in range(count)
    ]
    fars = [
        pltpu.make_async_remote_copy(
            block(which, layer, first + t * tile, tile, me ^ 3), got.at[pl.ds(t * tile, tile)],
            got_send.at[t], got_recv.at[t], device_id=partner, device_id_type=MESH)
        for t in range(count)
    ]
    beside = [
        pltpu.make_async_remote_copy(
            block(*SUMS[c], me ^ 1), near_refs[i], near_send.at[i], near_recv.at[i], device_id=partner, device_id_type=MESH)
        for i, c in enumerate(nears)
    ]
    outs = [pltpu.make_async_copy(total.at[pl.ds(t * tile, tile)], both.at[pl.ds(t * tile, tile)], out_sem.at[t]) for t in range(count)]
    pl.semaphore_wait(barrier, 1)
    for far, own in zip(fars, owns):
        far.start()
        own.start()
    for copy in beside:
        copy.start()
    for t in range(count):
        owns[t].wait()
        fars[t].wait_recv()
        here = pl.ds(t * tile, tile)
        total[here] = (got[here].astype(jnp.float32) + mine[here].astype(jnp.float32)).astype(jnp.bfloat16)
        outs[t].start()
    for t in range(count):
        fars[t].wait_send()
        outs[t].wait()
    for copy in beside:
        copy.wait()


def first_pair_body(chunk, terms, both, got, mine, send_sem, recv_sem, in_sem):
    _, layer, first, rows = chunk
    me = lax.axis_index("dp")
    partner = {"dp": me ^ 1}
    barrier = pltpu.get_barrier_semaphore()
    pl.semaphore_signal(barrier, inc=1, device_id=partner, device_id_type=MESH)

    def block(owner):
        size = terms.shape[2] // 4
        return terms.at[0, layer, pl.ds(pl.multiple_of(owner * size + first, 16), rows)]

    own = pltpu.make_async_copy(block(me ^ 2), mine, in_sem)
    far = pltpu.make_async_remote_copy(block(me ^ 3), got, send_sem, recv_sem, device_id=partner, device_id_type=MESH)
    own.start()
    pl.semaphore_wait(barrier, 1)
    far.start()
    own.wait()
    far.wait_recv()
    both[...] = (got[...].astype(jnp.float32) + mine[...].astype(jnp.float32)).astype(jnp.bfloat16)
    far.wait_send()


def first_pair(terms):
    which, _, _, rows = SUMS[0]
    cols = terms[which].shape[3]
    return pl.pallas_call(
        functools.partial(first_pair_body, SUMS[0]),
        in_specs=[pl.BlockSpec(memory_space=pltpu.HBM)],
        out_specs=pl.BlockSpec(memory_space=pltpu.VMEM),
        out_shape=jax.ShapeDtypeStruct((rows, cols), jnp.bfloat16),
        scratch_shapes=[pltpu.VMEM((rows, cols), jnp.bfloat16)] * 2 + [pltpu.SemaphoreType.DMA] * 3,
        compiler_params=pltpu.CompilerParams(collective_id=0, has_side_effects=True, vmem_limit_bytes=52 * 2**20),
        cost_estimate=pl.CostEstimate(flops=rows * cols, bytes_accessed=8 * rows * cols, transcendentals=0),
        name="first_pair",
    )(terms[which])


def pair_tile(rows, cols):
    return rows if rows * cols <= 96 * 3072 else math.gcd(rows, 64 * 3072 // cols)


def pair(terms, index, nears):
    chunk = SUMS[index]
    which, _, _, rows = chunk
    cols = terms[which].shape[3]
    count = rows // pair_tile(rows, cols)
    anywhere = pl.BlockSpec(memory_space=pl.ANY)
    shapes = [(rows, cols)] + [(SUMS[c][3], terms[SUMS[c][0]].shape[3]) for c in nears]
    return pl.pallas_call(
        functools.partial(pair_body, chunk, nears),
        in_specs=[anywhere] * 3,
        out_specs=[anywhere] * len(shapes),
        out_shape=[jax.ShapeDtypeStruct(shape, jnp.bfloat16) for shape in shapes],
        scratch_shapes=[pltpu.VMEM((rows, cols), jnp.bfloat16)] * 3
        + [pltpu.SemaphoreType.DMA((count,))] * 4
        + [pltpu.SemaphoreType.DMA((max(1, len(nears)),))] * 2,
        compiler_params=pltpu.CompilerParams(collective_id=index, has_side_effects=True),
        cost_estimate=pl.CostEstimate(flops=rows * cols, bytes_accessed=10 * rows * cols, transcendentals=0),
        name="pair",
    )(*terms)


def adamw_body(n_alias, me, own, near, far, w, m, v, *rest):
    send, out, m_out, v_out = rest[n_alias:]
    g = own[...].astype(jnp.float32) + near[...].astype(jnp.float32) + far[...].astype(jnp.float32)
    g = g.reshape(m.shape).astype(jnp.bfloat16).astype(jnp.float32)
    m_new = 0.9 * m[...] + 0.1 * g
    v_new = 0.95 * v[...] + 0.05 * g * g
    w_old = w[...].astype(jnp.float32)
    new = (w_old - 0.02 * (m_new * lax.rsqrt(v_new + 1e-8) + 0.1 * w_old)).astype(jnp.bfloat16)
    send[...] = new.reshape(send.shape)
    out[...] = new
    m_out[...] = m_new
    v_out[...] = v_new


def adamw(me, terms, near, far, w, m, v, step, before):
    r, c, first, rows = step
    _, layer, sum_first, _ = SUMS[r]
    _, _, chunk_first, chunk_rows = CHUNKS[c]
    block, cols = m.shape[1], m.shape[2]
    tile = math.gcd(rows, first, block, first - sum_first, first - chunk_first, 128 * 3072 // cols)
    at, per = first // tile, block // tile
    of_sum, of_chunk = (first - sum_first) // tile, (first - chunk_first) // tile
    mine = pl.BlockSpec((1, tile, cols), lambda i, me: (layer, at + i, 0))
    whole = pl.BlockSpec((1, tile, cols), lambda i, me: (layer, me[0] * per + at + i, 0))
    term = pl.BlockSpec((1, 1, tile, cols), lambda i, me: (0, layer, me[0] * per + at + i, 0))
    sums = pl.BlockSpec((tile, cols), lambda i, me: (of_sum + i, 0))
    chunk = pl.BlockSpec((tile, cols), lambda i, me: (of_chunk + i, 0))
    anywhere = pl.BlockSpec(memory_space=pl.ANY)
    have = [i for i, array in enumerate(before) if array is not None]
    size = rows * cols
    return pl.pallas_call(
        functools.partial(adamw_body, len(have)),
        grid_spec=pltpu.PrefetchScalarGridSpec(
            num_scalar_prefetch=1,
            grid=(rows // tile,),
            in_specs=[term, sums, sums, whole, mine, mine] + [anywhere] * len(have),
            out_specs=[chunk, whole, mine, mine],
        ),
        out_shape=[
            jax.ShapeDtypeStruct((chunk_rows, cols), jnp.bfloat16),
            jax.ShapeDtypeStruct(w.shape, jnp.bfloat16),
            jax.ShapeDtypeStruct(m.shape, jnp.float32),
            jax.ShapeDtypeStruct(v.shape, jnp.float32),
        ],
        input_output_aliases={7 + n: i for n, i in enumerate(have)},
        cost_estimate=pl.CostEstimate(flops=14 * size, bytes_accessed=28 * size, transcendentals=size),
        name="adamw",
    )(me, terms, near, far, w, m, v, *(before[i] for i in have))


def place_body(what, block, me, *refs):
    pieces, (_, out, sem) = refs[:-3], refs[-3:]
    copies = []
    for i, ((c, other), src) in enumerate(zip(what, pieces, strict=True)):
        _, layer, first, rows = CHUNKS[c]
        to = out.at[layer, pl.ds(pl.multiple_of((me[0] ^ other) * block + first, 16), rows)]
        copies.append(pltpu.make_async_copy(src, to, sem.at[i]))
    for copy in copies:
        copy.start()
    for copy in copies:
        copy.wait()


def place(me, what, pieces, out, block):
    size = sum(piece.size for piece in pieces)
    anywhere = pl.BlockSpec(memory_space=pl.ANY)
    n = len(pieces)
    return pl.pallas_call(
        functools.partial(place_body, what, block),
        in_specs=[pl.BlockSpec(memory_space=pltpu.SMEM)] + [pl.BlockSpec(memory_space=pltpu.VMEM)] * n + [anywhere],
        out_specs=anywhere,
        out_shape=jax.ShapeDtypeStruct(out.shape, out.dtype),
        input_output_aliases={1 + n: 0},
        scratch_shapes=[pltpu.SemaphoreType.DMA((n,))],
        compiler_params=pltpu.CompilerParams(vmem_limit_bytes=16 * 2**20),
        cost_estimate=pl.CostEstimate(flops=size, bytes_accessed=4 * size, transcendentals=0),
        name="place",
    )(me, *pieces, out)


def carry_body(chunk, block, me, beside, across, corner, before, out, held, in_sem, out_sem):
    _, layer, first, rows = chunk
    ins = [pltpu.make_async_copy(src, held.at[i], in_sem.at[i]) for i, src in enumerate((beside, across, corner))]
    outs = [
        pltpu.make_async_copy(held.at[i], out.at[layer, pl.ds(pl.multiple_of((me[0] ^ (1 + i)) * block + first, 16), rows)], out_sem.at[i])
        for i in range(3)
    ]
    for copy in ins:
        copy.start()
    for came, goes in zip(ins, outs):
        came.wait()
        goes.start()
    for copy in outs:
        copy.wait()


def carry(me, chunk, pieces, out, block):
    _, _, _, rows = chunk
    cols = out.shape[2]
    anywhere = pl.BlockSpec(memory_space=pl.ANY)
    return pl.pallas_call(
        functools.partial(carry_body, chunk, block),
        in_specs=[pl.BlockSpec(memory_space=pltpu.SMEM)] + [anywhere] * 4,
        out_specs=anywhere,
        out_shape=jax.ShapeDtypeStruct(out.shape, out.dtype),
        input_output_aliases={4: 0},
        scratch_shapes=[
            pltpu.VMEM((3, rows, cols), jnp.bfloat16),
            pltpu.SemaphoreType.DMA((3,)),
            pltpu.SemaphoreType.DMA((3,)),
        ],
        cost_estimate=pl.CostEstimate(flops=3 * rows * cols, bytes_accessed=12 * rows * cols, transcendentals=0),
        name="carry",
    )(me, *pieces, out)


def solution(mesh):
    def inner(*arrays):
        terms, weights, m, v = (arrays[i : i + 3] for i in (0, 3, 6, 9))
        me = lax.axis_index("dp").astype(jnp.int32).reshape(1)

        def send(x, to):
            return lax.ppermute(x, "dp", to)

        arrived, near = [], []
        for r in range(len(SUMS)):
            both, *more = pair(terms, r, () if r < 3 else (0, 1, 2, 3) if r == 3 else (r,)) if r else (first_pair(terms),)
            near += more
            arrived.append(send(both, ACROSS))

        state = [[None] * 3 for _ in weights]
        new = [None] * len(CHUNKS)
        for step in STEPS:
            r, c, _, _ = step
            which = SUMS[r][0]
            new[c], *state[which] = adamw(
                me, terms[which], near[r], arrived[r], weights[which], m[which], v[which], step, (new[c], *state[which]))
        across, beside, corner = [], [], []
        for c in range(len(CHUNKS)):
            across.append(send(new[c], ACROSS))
            beside.append(send(new[c], BESIDE))
        for c in range(len(CHUNKS)):
            corner.append(send(across[c], BESIDE))
        came = {1: beside, 2: across, 3: corner}
        for c in range(LAST):
            which = CHUNKS[c][0]
            what = ((c, 1), (c, 2), (c, 3))
            if c == LAST - 2:
                what += ((LAST - 1, 1), (LAST, 1))
            if c == LAST - 1:
                what = ((c, 2), (c, 3), (LAST, 2))
            pieces = [came[other][i] for i, other in what]
            if c < LAST - 2:
                state[which][0] = carry(me, CHUNKS[c], pieces, state[which][0], m[which].shape[1])
            else:
                state[which][0] = place(me, what, pieces, state[which][0], m[which].shape[1])
        which, layer, first, _ = CHUNKS[LAST]
        row = (lax.axis_index("dp") ^ 3) * m[which].shape[1] + first
        state[which][0] = lax.dynamic_update_slice(state[which][0], corner[LAST][None], (layer, row, 0))
        return tuple(state[which][i] for i in range(3) for which in range(3))

    all_of, cut_rows = P(None, None, None), P(None, "dp", None)
    return jax.shard_map(
        inner,
        mesh=mesh,
        in_specs=(P(("rep", "dp"), None, None, None),) * 3 + (all_of,) * 3 + (cut_rows,) * 6,
        out_specs=(P("rep", None, None),) * 3 + (P("rep", "dp", None),) * 6,
        check_vma=False,
    )
```

```python
import functools
import math

import jax
import jax.numpy as jnp
from jax import lax
from jax.experimental import pallas as pl
from jax.experimental.pallas import tpu as pltpu
from jax.sharding import PartitionSpec as P


ACROSS = [(0, 2), (2, 0), (1, 3), (3, 1)]
BESIDE = [(0, 1), (1, 0), (2, 3), (3, 2)]

SUMS = (
    (0, 0, 0, 32), (0, 0, 32, 32), (0, 0, 64, 64), (0, 0, 128, 128), (0, 1, 0, 256),
    (1, 0, 0, 256), (1, 1, 0, 256), (2, 0, 0, 768), (2, 1, 0, 768),
)
CHUNKS = (
    (0, 0, 0, 256), (0, 1, 0, 256), (1, 0, 0, 256), (1, 1, 0, 256),
    (2, 0, 0, 768), (2, 1, 0, 384), (2, 1, 384, 192), (2, 1, 576, 96), (2, 1, 672, 48), (2, 1, 720, 48),
)
STEPS = tuple(
    (r, c, max(sums[2], chunk[2]), min(sums[3], chunk[3]))
    for r, sums in enumerate(SUMS)
    for c, chunk in enumerate(CHUNKS)
    if sums[:2] == chunk[:2] and sums[2] < chunk[2] + chunk[3] and chunk[2] < sums[2] + sums[3]
)
LAST = len(CHUNKS) - 1
MESH = pl.DeviceIdType.MESH


def pair_body(chunk, nears, *refs):
    n = len(nears)
    terms, (both, *near_refs) = refs[:3], refs[3 : 4 + n]
    got, mine, total, got_send, got_recv, in_sem, out_sem, near_send, near_recv = refs[4 + n :]
    which, layer, first, rows = chunk
    me = lax.axis_index("dp")
    partner = {"dp": me ^ 1}
    barrier = pltpu.get_barrier_semaphore()
    pl.semaphore_signal(barrier, inc=1, device_id=partner, device_id_type=MESH)

    def block(which, layer, first, rows, owner):
        size = terms[which].shape[2] // 4
        return terms[which].at[0, layer, pl.ds(pl.multiple_of(owner * size + first, 16), rows)]

    tile = pair_tile(rows, terms[which].shape[3])
    count = rows // tile
    owns = [
        pltpu.make_async_copy(block(which, layer, first + t * tile, tile, me ^ 2), mine.at[pl.ds(t * tile, tile)], in_sem.at[t])
        for t in range(count)
    ]
    fars = [
        pltpu.make_async_remote_copy(
            block(which, layer, first + t * tile, tile, me ^ 3), got.at[pl.ds(t * tile, tile)],
            got_send.at[t], got_recv.at[t], device_id=partner, device_id_type=MESH)
        for t in range(count)
    ]
    beside = [
        pltpu.make_async_remote_copy(
            block(*SUMS[c], me ^ 1), near_refs[i], near_send.at[i], near_recv.at[i], device_id=partner, device_id_type=MESH)
        for i, c in enumerate(nears)
    ]
    outs = [pltpu.make_async_copy(total.at[pl.ds(t * tile, tile)], both.at[pl.ds(t * tile, tile)], out_sem.at[t]) for t in range(count)]
    for own in owns:
        own.start()
    pl.semaphore_wait(barrier, 1)
    for far in fars:
        far.start()
    for copy in beside:
        copy.start()
    for t in range(count):
        fars[t].wait_recv()
        owns[t].wait()
        here = pl.ds(t * tile, tile)
        total[here] = (got[here].astype(jnp.float32) + mine[here].astype(jnp.float32)).astype(jnp.bfloat16)
        outs[t].start()
    for t in range(count):
        fars[t].wait_send()
        outs[t].wait()
    for copy in beside:
        copy.wait()


def first_pair_body(chunk, terms, both, got, mine, send_sem, recv_sem, in_sem):
    _, layer, first, rows = chunk
    me = lax.axis_index("dp")
    partner = {"dp": me ^ 1}
    barrier = pltpu.get_barrier_semaphore()
    pl.semaphore_signal(barrier, inc=1, device_id=partner, device_id_type=MESH)

    def block(owner):
        size = terms.shape[2] // 4
        return terms.at[0, layer, pl.ds(pl.multiple_of(owner * size + first, 16), rows)]

    own = pltpu.make_async_copy(block(me ^ 2), mine, in_sem)
    far = pltpu.make_async_remote_copy(block(me ^ 3), got, send_sem, recv_sem, device_id=partner, device_id_type=MESH)
    own.start()
    pl.semaphore_wait(barrier, 1)
    far.start()
    far.wait_recv()
    own.wait()
    both[...] = (got[...].astype(jnp.float32) + mine[...].astype(jnp.float32)).astype(jnp.bfloat16)
    far.wait_send()


def first_pair(terms):
    which, _, _, rows = SUMS[0]
    cols = terms[which].shape[3]
    return pl.pallas_call(
        functools.partial(first_pair_body, SUMS[0]),
        in_specs=[pl.BlockSpec(memory_space=pltpu.HBM)],
        out_specs=pl.BlockSpec(memory_space=pltpu.VMEM),
        out_shape=jax.ShapeDtypeStruct((rows, cols), jnp.bfloat16),
        scratch_shapes=[pltpu.VMEM((rows, cols), jnp.bfloat16)] * 2 + [pltpu.SemaphoreType.DMA] * 3,
        compiler_params=pltpu.CompilerParams(collective_id=0, has_side_effects=True, vmem_limit_bytes=52 * 2**20),
        cost_estimate=pl.CostEstimate(flops=rows * cols, bytes_accessed=8 * rows * cols, transcendentals=0),
        name="first_pair",
    )(terms[which])


def pair_tile(rows, cols):
    return rows if rows * cols <= 96 * 3072 else math.gcd(rows, 64 * 3072 // cols)


def pair(terms, index, nears):
    chunk = SUMS[index]
    which, _, _, rows = chunk
    cols = terms[which].shape[3]
    count = rows // pair_tile(rows, cols)
    anywhere = pl.BlockSpec(memory_space=pl.ANY)
    shapes = [(rows, cols)] + [(SUMS[c][3], terms[SUMS[c][0]].shape[3]) for c in nears]
    return pl.pallas_call(
        functools.partial(pair_body, chunk, nears),
        in_specs=[anywhere] * 3,
        out_specs=[anywhere] * len(shapes),
        out_shape=[jax.ShapeDtypeStruct(shape, jnp.bfloat16) for shape in shapes],
        scratch_shapes=[pltpu.VMEM((rows, cols), jnp.bfloat16)] * 3
        + [pltpu.SemaphoreType.DMA((count,))] * 4
        + [pltpu.SemaphoreType.DMA((max(1, len(nears)),))] * 2,
        compiler_params=pltpu.CompilerParams(collective_id=index, has_side_effects=True),
        cost_estimate=pl.CostEstimate(flops=rows * cols, bytes_accessed=10 * rows * cols, transcendentals=0),
        name="pair",
    )(*terms)


def adamw_body(n_alias, me, own, near, far, w, m, v, *rest):
    send, out, m_out, v_out = rest[n_alias:]
    g = own[...].astype(jnp.float32) + near[...].astype(jnp.float32) + far[...].astype(jnp.float32)
    g = g.reshape(m.shape).astype(jnp.bfloat16).astype(jnp.float32)
    m_new = 0.9 * m[...] + 0.1 * g
    v_new = 0.95 * v[...] + 0.05 * g * g
    w_old = w[...].astype(jnp.float32)
    new = (w_old - 0.02 * (m_new * lax.rsqrt(v_new + 1e-8) + 0.1 * w_old)).astype(jnp.bfloat16)
    send[...] = new.reshape(send.shape)
    out[...] = new
    m_out[...] = m_new
    v_out[...] = v_new


def adamw(me, terms, near, far, w, m, v, step, before):
    r, c, first, rows = step
    _, layer, sum_first, _ = SUMS[r]
    _, _, chunk_first, chunk_rows = CHUNKS[c]
    block, cols = m.shape[1], m.shape[2]
    tile = math.gcd(rows, first, block, first - sum_first, first - chunk_first, 64 * 3072 // cols)
    at, per = first // tile, block // tile
    of_sum, of_chunk = (first - sum_first) // tile, (first - chunk_first) // tile
    mine = pl.BlockSpec((1, tile, cols), lambda i, me: (layer, at + i, 0))
    whole = pl.BlockSpec((1, tile, cols), lambda i, me: (layer, me[0] * per + at + i, 0))
    term = pl.BlockSpec((1, 1, tile, cols), lambda i, me: (0, layer, me[0] * per + at + i, 0))
    sums = pl.BlockSpec((tile, cols), lambda i, me: (of_sum + i, 0))
    chunk = pl.BlockSpec((tile, cols), lambda i, me: (of_chunk + i, 0))
    anywhere = pl.BlockSpec(memory_space=pl.ANY)
    have = [i for i, array in enumerate(before) if array is not None]
    size = rows * cols
    return pl.pallas_call(
        functools.partial(adamw_body, len(have)),
        grid_spec=pltpu.PrefetchScalarGridSpec(
            num_scalar_prefetch=1,
            grid=(rows // tile,),
            in_specs=[term, sums, sums, whole, mine, mine] + [anywhere] * len(have),
            out_specs=[chunk, whole, mine, mine],
        ),
        out_shape=[
            jax.ShapeDtypeStruct((chunk_rows, cols), jnp.bfloat16),
            jax.ShapeDtypeStruct(w.shape, jnp.bfloat16),
            jax.ShapeDtypeStruct(m.shape, jnp.float32),
            jax.ShapeDtypeStruct(v.shape, jnp.float32),
        ],
        input_output_aliases={7 + n: i for n, i in enumerate(have)},
        cost_estimate=pl.CostEstimate(flops=14 * size, bytes_accessed=28 * size, transcendentals=size),
        name="adamw",
    )(me, terms, near, far, w, m, v, *(before[i] for i in have))


def place_body(what, block, me, *refs):
    pieces, (_, out, sem) = refs[:-3], refs[-3:]
    copies = []
    for i, ((c, other), src) in enumerate(zip(what, pieces, strict=True)):
        _, layer, first, rows = CHUNKS[c]
        to = out.at[layer, pl.ds(pl.multiple_of((me[0] ^ other) * block + first, 16), rows)]
        copies.append(pltpu.make_async_copy(src, to, sem.at[i]))
    for copy in copies:
        copy.start()
    for copy in copies:
        copy.wait()


def place(me, what, pieces, out, block):
    size = sum(piece.size for piece in pieces)
    anywhere = pl.BlockSpec(memory_space=pl.ANY)
    n = len(pieces)
    return pl.pallas_call(
        functools.partial(place_body, what, block),
        in_specs=[pl.BlockSpec(memory_space=pltpu.SMEM)] + [pl.BlockSpec(memory_space=pltpu.VMEM)] * n + [anywhere],
        out_specs=anywhere,
        out_shape=jax.ShapeDtypeStruct(out.shape, out.dtype),
        input_output_aliases={1 + n: 0},
        scratch_shapes=[pltpu.SemaphoreType.DMA((n,))],
        compiler_params=pltpu.CompilerParams(vmem_limit_bytes=16 * 2**20),
        cost_estimate=pl.CostEstimate(flops=size, bytes_accessed=4 * size, transcendentals=0),
        name="place",
    )(me, *pieces, out)


def carry_body(chunks, block, me, *refs):
    n = 3 * len(chunks)
    pieces, (_, out, held, in_sem, out_sem) = refs[:n], refs[n:]
    ins, outs = [], []
    for i, src in enumerate(pieces):
        _, layer, first, rows = chunks[i // 3]
        to = out.at[layer, pl.ds(pl.multiple_of((me[0] ^ (1 + i % 3)) * block + first, 16), rows)]
        ins.append(pltpu.make_async_copy(src, held.at[i], in_sem.at[i]))
        outs.append(pltpu.make_async_copy(held.at[i], to, out_sem.at[i]))
    for copy in ins:
        copy.start()
    for came, goes in zip(ins, outs):
        came.wait()
        goes.start()
    for copy in outs:
        copy.wait()


def carry(me, chunks, pieces, out, block):
    rows, cols = pieces[0].shape
    n = len(pieces)
    anywhere = pl.BlockSpec(memory_space=pl.ANY)
    return pl.pallas_call(
        functools.partial(carry_body, chunks, block),
        in_specs=[pl.BlockSpec(memory_space=pltpu.SMEM)] + [anywhere] * (n + 1),
        out_specs=anywhere,
        out_shape=jax.ShapeDtypeStruct(out.shape, out.dtype),
        input_output_aliases={1 + n: 0},
        scratch_shapes=[
            pltpu.VMEM((n, rows, cols), jnp.bfloat16),
            pltpu.SemaphoreType.DMA((n,)),
            pltpu.SemaphoreType.DMA((n,)),
        ],
        cost_estimate=pl.CostEstimate(flops=n * rows * cols, bytes_accessed=4 * n * rows * cols, transcendentals=0),
        name="carry",
    )(me, *pieces, out)


def solution(mesh):
    def inner(*arrays):
        terms, weights, m, v = (arrays[i : i + 3] for i in (0, 3, 6, 9))
        me = lax.axis_index("dp").astype(jnp.int32).reshape(1)

        def send(x, to):
            return lax.ppermute(x, "dp", to)

        arrived, near = [], []
        for r in range(len(SUMS)):
            both, *more = pair(terms, r, () if r < 3 else (0, 1, 2, 3) if r == 3 else (r,)) if r else (first_pair(terms),)
            near += more
            arrived.append(send(both, ACROSS))

        state = [[None] * 3 for _ in weights]
        new = [None] * len(CHUNKS)
        for step in STEPS:
            r, c, _, _ = step
            which = SUMS[r][0]
            new[c], *state[which] = adamw(
                me, terms[which], near[r], arrived[r], weights[which], m[which], v[which], step, (new[c], *state[which]))
        across, beside, corner = [], [], []
        for c in range(len(CHUNKS)):
            across.append(send(new[c], ACROSS))
            beside.append(send(new[c], BESIDE))
        for c in range(len(CHUNKS)):
            corner.append(send(across[c], BESIDE))
        came = {1: beside, 2: across, 3: corner}
        for c in range(LAST):
            which = CHUNKS[c][0]
            what = ((c, 1), (c, 2), (c, 3))
            if c == LAST - 2:
                what += ((LAST - 1, 1), (LAST, 1))
            if c == LAST - 1:
                what = ((c, 2), (c, 3), (LAST, 2))
            if c in (0, 2):
                continue
            if c in (1, 3):
                what = ((c - 1, 1), (c - 1, 2), (c - 1, 3)) + what
            pieces = [came[other][i] for i, other in what]
            if c < LAST - 2:
                state[which][0] = carry(me, [CHUNKS[i] for i, _ in what[::3]], pieces, state[which][0], m[which].shape[1])
            else:
                state[which][0] = place(me, what, pieces, state[which][0], m[which].shape[1])
        which, layer, first, _ = CHUNKS[LAST]
        row = (lax.axis_index("dp") ^ 3) * m[which].shape[1] + first
        state[which][0] = lax.dynamic_update_slice(state[which][0], corner[LAST][None], (layer, row, 0))
        return tuple(state[which][i] for i in range(3) for which in range(3))

    all_of, cut_rows = P(None, None, None), P(None, "dp", None)
    return jax.shard_map(
        inner,
        mesh=mesh,
        in_specs=(P(("rep", "dp"), None, None, None),) * 3 + (all_of,) * 3 + (cut_rows,) * 6,
        out_specs=(P("rep", None, None),) * 3 + (P("rep", "dp", None),) * 6,
        check_vma=False,
    )
```

```python
import functools
import math

import jax
import jax.numpy as jnp
from jax import lax
from jax.experimental import pallas as pl
from jax.experimental.pallas import tpu as pltpu
from jax.sharding import PartitionSpec as P


ACROSS = [(0, 2), (2, 0), (1, 3), (3, 1)]
BESIDE = [(0, 1), (1, 0), (2, 3), (3, 2)]

SUMS = (
    (0, 0, 0, 32), (0, 0, 32, 32), (0, 0, 64, 64), (0, 0, 128, 128), (0, 1, 0, 256),
    (1, 0, 0, 256), (1, 1, 0, 256), (2, 0, 0, 768), (2, 1, 0, 768),
)
CHUNKS = (
    (0, 0, 0, 256), (0, 1, 0, 256), (1, 0, 0, 256), (1, 1, 0, 256),
    (2, 0, 0, 768), (2, 1, 0, 384), (2, 1, 384, 192), (2, 1, 576, 96), (2, 1, 672, 48), (2, 1, 720, 48),
)
STEPS = tuple(
    (r, c, max(sums[2], chunk[2]), min(sums[3], chunk[3]))
    for r, sums in enumerate(SUMS)
    for c, chunk in enumerate(CHUNKS)
    if sums[:2] == chunk[:2] and sums[2] < chunk[2] + chunk[3] and chunk[2] < sums[2] + sums[3]
)
LAST = len(CHUNKS) - 1
MESH = pl.DeviceIdType.MESH


def pair_body(chunk, nears, *refs):
    n = len(nears)
    terms, (both, *near_refs) = refs[:3], refs[3 : 4 + n]
    got, mine, total, got_send, got_recv, in_sem, out_sem, near_send, near_recv = refs[4 + n :]
    which, layer, first, rows = chunk
    me = lax.axis_index("dp")
    partner = {"dp": me ^ 1}
    barrier = pltpu.get_barrier_semaphore()
    pl.semaphore_signal(barrier, inc=1, device_id=partner, device_id_type=MESH)

    def block(which, layer, first, rows, owner):
        size = terms[which].shape[2] // 4
        return terms[which].at[0, layer, pl.ds(pl.multiple_of(owner * size + first, 16), rows)]

    tile = pair_tile(rows, terms[which].shape[3])
    count = rows // tile
    owns = [
        pltpu.make_async_copy(block(which, layer, first + t * tile, tile, me ^ 2), mine.at[pl.ds(t * tile, tile)], in_sem.at[t])
        for t in range(count)
    ]
    fars = [
        pltpu.make_async_remote_copy(
            block(which, layer, first + t * tile, tile, me ^ 3), got.at[pl.ds(t * tile, tile)],
            got_send.at[t], got_recv.at[t], device_id=partner, device_id_type=MESH)
        for t in range(count)
    ]
    beside = [
        pltpu.make_async_remote_copy(
            block(*SUMS[c], me ^ 1), near_refs[i], near_send.at[i], near_recv.at[i], device_id=partner, device_id_type=MESH)
        for i, c in enumerate(nears)
    ]
    outs = [pltpu.make_async_copy(total.at[pl.ds(t * tile, tile)], both.at[pl.ds(t * tile, tile)], out_sem.at[t]) for t in range(count)]
    for own in owns:
        own.start()
    pl.semaphore_wait(barrier, 1)
    for far in fars:
        far.start()
    for copy in beside:
        copy.start()
    for t in range(count):
        fars[t].wait_recv()
        owns[t].wait()
        here = pl.ds(t * tile, tile)
        total[here] = (got[here].astype(jnp.float32) + mine[here].astype(jnp.float32)).astype(jnp.bfloat16)
        outs[t].start()
    for t in range(count):
        fars[t].wait_send()
        outs[t].wait()
    for copy in beside:
        copy.wait()


def first_pair_body(chunk, terms, both, got, mine, send_sem, recv_sem, in_sem):
    _, layer, first, rows = chunk
    me = lax.axis_index("dp")
    partner = {"dp": me ^ 1}
    barrier = pltpu.get_barrier_semaphore()
    pl.semaphore_signal(barrier, inc=1, device_id=partner, device_id_type=MESH)

    def block(owner):
        size = terms.shape[2] // 4
        return terms.at[0, layer, pl.ds(pl.multiple_of(owner * size + first, 16), rows)]

    own = pltpu.make_async_copy(block(me ^ 2), mine, in_sem)
    far = pltpu.make_async_remote_copy(block(me ^ 3), got, send_sem, recv_sem, device_id=partner, device_id_type=MESH)
    own.start()
    pl.semaphore_wait(barrier, 1)
    far.start()
    far.wait_recv()
    own.wait()
    both[...] = (got[...].astype(jnp.float32) + mine[...].astype(jnp.float32)).astype(jnp.bfloat16)
    far.wait_send()


def first_pair(terms):
    which, _, _, rows = SUMS[0]
    cols = terms[which].shape[3]
    return pl.pallas_call(
        functools.partial(first_pair_body, SUMS[0]),
        in_specs=[pl.BlockSpec(memory_space=pltpu.HBM)],
        out_specs=pl.BlockSpec(memory_space=pltpu.VMEM),
        out_shape=jax.ShapeDtypeStruct((rows, cols), jnp.bfloat16),
        scratch_shapes=[pltpu.VMEM((rows, cols), jnp.bfloat16)] * 2 + [pltpu.SemaphoreType.DMA] * 3,
        compiler_params=pltpu.CompilerParams(collective_id=0, has_side_effects=True, vmem_limit_bytes=52 * 2**20),
        cost_estimate=pl.CostEstimate(flops=rows * cols, bytes_accessed=8 * rows * cols, transcendentals=0),
        name="first_pair",
    )(terms[which])


def pair_tile(rows, cols):
    return rows if rows * cols <= 96 * 3072 else math.gcd(rows, 128 * 3072 // cols)


def pair(terms, index, nears):
    chunk = SUMS[index]
    which, _, _, rows = chunk
    cols = terms[which].shape[3]
    count = rows // pair_tile(rows, cols)
    anywhere = pl.BlockSpec(memory_space=pl.ANY)
    shapes = [(rows, cols)] + [(SUMS[c][3], terms[SUMS[c][0]].shape[3]) for c in nears]
    return pl.pallas_call(
        functools.partial(pair_body, chunk, nears),
        in_specs=[anywhere] * 3,
        out_specs=[anywhere] * len(shapes),
        out_shape=[jax.ShapeDtypeStruct(shape, jnp.bfloat16) for shape in shapes],
        scratch_shapes=[pltpu.VMEM((rows, cols), jnp.bfloat16)] * 3
        + [pltpu.SemaphoreType.DMA((count,))] * 4
        + [pltpu.SemaphoreType.DMA((max(1, len(nears)),))] * 2,
        compiler_params=pltpu.CompilerParams(collective_id=index, has_side_effects=True),
        cost_estimate=pl.CostEstimate(flops=rows * cols, bytes_accessed=10 * rows * cols, transcendentals=0),
        name="pair",
    )(*terms)


def adamw_body(n_alias, me, own, near, far, w, m, v, *rest):
    send, out, m_out, v_out = rest[n_alias:]
    g = own[...].astype(jnp.float32) + near[...].astype(jnp.float32) + far[...].astype(jnp.float32)
    g = g.reshape(m.shape).astype(jnp.bfloat16).astype(jnp.float32)
    m_new = 0.9 * m[...] + 0.1 * g
    v_new = 0.95 * v[...] + 0.05 * g * g
    w_old = w[...].astype(jnp.float32)
    new = (w_old - 0.02 * (m_new * lax.rsqrt(v_new + 1e-8) + 0.1 * w_old)).astype(jnp.bfloat16)
    send[...] = new.reshape(send.shape)
    out[...] = new
    m_out[...] = m_new
    v_out[...] = v_new


def adamw(me, terms, near, far, w, m, v, step, before):
    r, c, first, rows = step
    _, layer, sum_first, _ = SUMS[r]
    _, _, chunk_first, chunk_rows = CHUNKS[c]
    block, cols = m.shape[1], m.shape[2]
    tile = math.gcd(rows, first, block, first - sum_first, first - chunk_first, 64 * 3072 // cols)
    at, per = first // tile, block // tile
    of_sum, of_chunk = (first - sum_first) // tile, (first - chunk_first) // tile
    mine = pl.BlockSpec((1, tile, cols), lambda i, me: (layer, at + i, 0))
    whole = pl.BlockSpec((1, tile, cols), lambda i, me: (layer, me[0] * per + at + i, 0))
    term = pl.BlockSpec((1, 1, tile, cols), lambda i, me: (0, layer, me[0] * per + at + i, 0))
    sums = pl.BlockSpec((tile, cols), lambda i, me: (of_sum + i, 0))
    chunk = pl.BlockSpec((tile, cols), lambda i, me: (of_chunk + i, 0))
    anywhere = pl.BlockSpec(memory_space=pl.ANY)
    have = [i for i, array in enumerate(before) if array is not None]
    size = rows * cols
    return pl.pallas_call(
        functools.partial(adamw_body, len(have)),
        grid_spec=pltpu.PrefetchScalarGridSpec(
            num_scalar_prefetch=1,
            grid=(rows // tile,),
            in_specs=[term, sums, sums, whole, mine, mine] + [anywhere] * len(have),
            out_specs=[chunk, whole, mine, mine],
        ),
        out_shape=[
            jax.ShapeDtypeStruct((chunk_rows, cols), jnp.bfloat16),
            jax.ShapeDtypeStruct(w.shape, jnp.bfloat16),
            jax.ShapeDtypeStruct(m.shape, jnp.float32),
            jax.ShapeDtypeStruct(v.shape, jnp.float32),
        ],
        input_output_aliases={7 + n: i for n, i in enumerate(have)},
        cost_estimate=pl.CostEstimate(flops=14 * size, bytes_accessed=28 * size, transcendentals=size),
        name="adamw",
    )(me, terms, near, far, w, m, v, *(before[i] for i in have))


def place_body(what, block, me, *refs):
    pieces, (_, out, sem) = refs[:-3], refs[-3:]
    copies = []
    for i, ((c, other), src) in enumerate(zip(what, pieces, strict=True)):
        _, layer, first, rows = CHUNKS[c]
        to = out.at[layer, pl.ds(pl.multiple_of((me[0] ^ other) * block + first, 16), rows)]
        copies.append(pltpu.make_async_copy(src, to, sem.at[i]))
    for copy in copies:
        copy.start()
    for copy in copies:
        copy.wait()


def place(me, what, pieces, out, block):
    size = sum(piece.size for piece in pieces)
    anywhere = pl.BlockSpec(memory_space=pl.ANY)
    n = len(pieces)
    return pl.pallas_call(
        functools.partial(place_body, what, block),
        in_specs=[pl.BlockSpec(memory_space=pltpu.SMEM)] + [pl.BlockSpec(memory_space=pltpu.VMEM)] * n + [anywhere],
        out_specs=anywhere,
        out_shape=jax.ShapeDtypeStruct(out.shape, out.dtype),
        input_output_aliases={1 + n: 0},
        scratch_shapes=[pltpu.SemaphoreType.DMA((n,))],
        compiler_params=pltpu.CompilerParams(vmem_limit_bytes=16 * 2**20),
        cost_estimate=pl.CostEstimate(flops=size, bytes_accessed=4 * size, transcendentals=0),
        name="place",
    )(me, *pieces, out)


def carry_body(chunk, block, me, beside, across, corner, before, out, held, in_sem, out_sem):
    _, layer, first, rows = chunk
    ins = [pltpu.make_async_copy(src, held.at[i], in_sem.at[i]) for i, src in enumerate((beside, across, corner))]
    outs = [
        pltpu.make_async_copy(held.at[i], out.at[layer, pl.ds(pl.multiple_of((me[0] ^ (1 + i)) * block + first, 16), rows)], out_sem.at[i])
        for i in range(3)
    ]
    for copy in ins:
        copy.start()
    for came, goes in zip(ins, outs):
        came.wait()
        goes.start()
    for copy in outs:
        copy.wait()


def carry(me, chunk, pieces, out, block):
    _, _, _, rows = chunk
    cols = out.shape[2]
    anywhere = pl.BlockSpec(memory_space=pl.ANY)
    return pl.pallas_call(
        functools.partial(carry_body, chunk, block),
        in_specs=[pl.BlockSpec(memory_space=pltpu.SMEM)] + [anywhere] * 4,
        out_specs=anywhere,
        out_shape=jax.ShapeDtypeStruct(out.shape, out.dtype),
        input_output_aliases={4: 0},
        scratch_shapes=[
            pltpu.VMEM((3, rows, cols), jnp.bfloat16),
            pltpu.SemaphoreType.DMA((3,)),
            pltpu.SemaphoreType.DMA((3,)),
        ],
        cost_estimate=pl.CostEstimate(flops=3 * rows * cols, bytes_accessed=12 * rows * cols, transcendentals=0),
        name="carry",
    )(me, *pieces, out)


def solution(mesh):
    def inner(*arrays):
        terms, weights, m, v = (arrays[i : i + 3] for i in (0, 3, 6, 9))
        me = lax.axis_index("dp").astype(jnp.int32).reshape(1)

        def send(x, to):
            return lax.ppermute(x, "dp", to)

        arrived, near = [], []
        for r in range(len(SUMS)):
            both, *more = pair(terms, r, () if r < 3 else (0, 1, 2, 3) if r == 3 else (r,)) if r else (first_pair(terms),)
            near += more
            arrived.append(send(both, ACROSS))

        state = [[None] * 3 for _ in weights]
        new = [None] * len(CHUNKS)
        for step in STEPS:
            r, c, _, _ = step
            which = SUMS[r][0]
            new[c], *state[which] = adamw(
                me, terms[which], near[r], arrived[r], weights[which], m[which], v[which], step, (new[c], *state[which]))
        across, beside, corner = [], [], []
        for c in range(len(CHUNKS)):
            across.append(send(new[c], ACROSS))
            beside.append(send(new[c], BESIDE))
        for c in range(len(CHUNKS)):
            corner.append(send(across[c], BESIDE))
        came = {1: beside, 2: across, 3: corner}
        for c in range(LAST):
            which = CHUNKS[c][0]
            what = ((c, 1), (c, 2), (c, 3))
            if c == LAST - 2:
                what += ((LAST - 1, 1), (LAST, 1))
            if c == LAST - 1:
                what = ((c, 2), (c, 3), (LAST, 2))
            pieces = [came[other][i] for i, other in what]
            if c < LAST - 2:
                state[which][0] = carry(me, CHUNKS[c], pieces, state[which][0], m[which].shape[1])
            else:
                state[which][0] = place(me, what, pieces, state[which][0], m[which].shape[1])
        which, layer, first, _ = CHUNKS[LAST]
        row = (lax.axis_index("dp") ^ 3) * m[which].shape[1] + first
        state[which][0] = lax.dynamic_update_slice(state[which][0], corner[LAST][None], (layer, row, 0))
        return tuple(state[which][i] for i in range(3) for which in range(3))

    all_of, cut_rows = P(None, None, None), P(None, "dp", None)
    return jax.shard_map(
        inner,
        mesh=mesh,
        in_specs=(P(("rep", "dp"), None, None, None),) * 3 + (all_of,) * 3 + (cut_rows,) * 6,
        out_specs=(P("rep", None, None),) * 3 + (P("rep", "dp", None),) * 6,
        check_vma=False,
    )
```
